32 devices in a mesh: gx: 8 (over z, x), gy: 4 (over y, core).
Axes of the slice: x: 2, y: 2, z: 4, core: 2. Of those that a mesh axis runs over, the one named last changes fastest.
Arguments:
- state: float32 [12, 4, 256, 1024], P(None, None, 'gy', 'gx'), may hold values from -240 to 240, as said below
- inverse: float32 [128, 256, 256], P('gy'), may hold values from -0.6 to 1.8, as said below
Outputs:
- updated: float32 [12, 4, 256, 1024], P(None, None, 'gy', 'gx')
- wall_stress: float32 [12, 2, 2, 1024], P(None, None, None, 'gx')
The draws below stay inside these ranges and needn't reach their ends.
Inputs may be any that keep to these rules, and one draw needn't show every extreme that they name: `state`: perturbation coefficients, of varying size over coefficients and x. Each inverse is a dense matrix with a positive diagonal.
All inputs are finite; a program needn't handle non-finite values.
Results may differ from the reference program's by a relative error of at most 0.0003.
Values sent between devices are 32-bit elements; how exact they have to be, the bound alone decides.
No kernel may reach another device: no remote copies, remote signals or barrier semaphores. Data moves between devices by JAX's collectives and lax.ppermute only.
A program may use at most 64 MiB of HBM per device.

```python
import jax
import jax.numpy as jnp
from jax import lax

NY = 256
MODES = 128
X_DEV = 128
HALO = 64
MEMBERS = 12
NX = 1024
N_GX = 8


def draw_state(key, part):
    keys = jax.random.split(jax.random.fold_in(key, 11), 2)
    shape = (MEMBERS, 4, NY, NX)
    x_fraction = jnp.arange(NX, dtype=jnp.float32) / NX
    y_fraction = jnp.arange(NY, dtype=jnp.float32) / NY
    envelope = (1.0 + 2.0 * x_fraction)[None, None, None, :] * (1.0 + 2.0 * y_fraction)[None, None, :, None]
    roughness = jax.random.uniform(keys[1], shape, minval=0.5, maxval=1.5)
    base_draw = jnp.clip(jax.random.normal(keys[0], shape), -4.0, 4.0)
    return (base_draw * roughness * envelope).astype(jnp.float32)


def draw_inverse(key, part):
    keys = jax.random.split(jax.random.fold_in(key, 23), 2)
    diagonal = jnp.exp(jax.random.uniform(keys[0], (MODES, NY), minval=jnp.log(0.4), maxval=jnp.log(1.2)))
    identity = jnp.eye(NY, dtype=jnp.float32)
    noise = jnp.clip(jax.random.normal(keys[1], (MODES, NY, NY)), -5.0, 5.0) * 0.6 / jnp.sqrt(1.0 * NY)
    return (noise + identity[None, :, :] * diagonal[:, :, None]).astype(jnp.float32)


def setup_inputs(seed: int = 0) -> dict:
    key_list = jax.random.split(jax.random.key(seed), 3)
    state = draw_state(jax.random.fold_in(key_list[2], 71), 0)
    inverse = draw_inverse(jax.random.fold_in(key_list[2], 71), 0)
    return {"state": state, "inverse": inverse}


EPSILON = 1e-06
TIME_STEP = 0.5
MEAN_FLOW = 0.8
CORIOLIS = 0.6
STRATIFICATION = 0.9
HIGHEST = lax.Precision.HIGHEST

def window_tables(window, rim_width, points, mode_count):
    position = jnp.arange(window, dtype=jnp.int32)
    mode_index = jnp.arange(mode_count, dtype=jnp.int32)
    half_count = mode_count // 2
    is_cosine = mode_index <= half_count
    wave_index = jnp.where(is_cosine, mode_index, mode_index - half_count)
    product_index = position[:, None] * wave_index[None, :] % window
    phases = 2.0 * jnp.pi * product_index.astype(jnp.float32) / window
    wave_float = wave_index.astype(jnp.float32)
    weights_norm = jnp.where(wave_index == 0, jnp.sqrt(1.0 / window), jnp.sqrt(2.0 / window))
    fourier_basis = jnp.where(is_cosine[None, :], jnp.cos(phases), jnp.sin(phases)) * weights_norm[None, :]
    wavenumber = 2.0 * jnp.pi * wave_float / window
    paired = wave_index[:, None] == wave_index[None, :]
    to_sine = is_cosine[:, None] & jnp.logical_not(is_cosine[None, :]) & paired
    to_cosine = jnp.logical_not(is_cosine[:, None]) & is_cosine[None, :] & paired
    derivative = jnp.where(to_sine, -wavenumber[:, None], 0.0) + jnp.where(to_cosine, wavenumber[:, None], 0.0)
    position_float = position.astype(jnp.float32)
    window_taper = 0.25 + 0.75 * jnp.sin(jnp.pi * (position_float + 0.5) / window) ** 2
    slopes = jnp.dot(fourier_basis, derivative, precision=HIGHEST, preferred_element_type=jnp.float32)
    projection = jnp.concatenate([fourier_basis, slopes], axis=1) * window_taper[:, None]
    back_table = (fourier_basis[rim_width:rim_width + points, :] / window_taper[rim_width:rim_width + points, None]).T
    return (projection, back_table)

def advance(spectra, mode_count, coef_global, coef_count):
    modal_coef = spectra[..., :mode_count]
    slope = spectra[..., mode_count:]
    rhs_first = modal_coef[:, 0] + TIME_STEP * (-MEAN_FLOW * slope[:, 0] + CORIOLIS * modal_coef[:, 2])
    rhs_second = modal_coef[:, 1] + TIME_STEP * (-MEAN_FLOW * slope[:, 1] + modal_coef[:, 3])
    rhs_third = modal_coef[:, 2] + TIME_STEP * (-MEAN_FLOW * slope[:, 2] - CORIOLIS * modal_coef[:, 0])
    rhs_fourth = modal_coef[:, 3] + TIME_STEP * (-MEAN_FLOW * slope[:, 3] - STRATIFICATION * modal_coef[:, 1])
    stacked = jnp.stack([rhs_first, rhs_second, rhs_third, rhs_fourth], axis=1)
    interior = (coef_global < coef_count - 2)[None, None, :, None]
    return jnp.where(interior, stacked, 0.0)

def wall_weights(coef_global, coef_count):
    coef_float = coef_global.astype(jnp.float32)
    curvature = coef_float * coef_float / (coef_count * coef_count)
    parity = jnp.where(coef_global % 2 == 0, -1.0, 1.0)
    return jnp.stack([curvature, parity * curvature])

def reference(state, inverse):
    members, fields, coef_count, grid_x = state.shape
    window = X_DEV + 2 * HALO
    projection, back_table = window_tables(window, HALO, X_DEV, MODES)
    norm_sum = lax.optimization_barrier(jnp.sum(state * state, axis=(1, 2, 3)))
    renorm = lax.rsqrt(norm_sum / (fields * coef_count * grid_x) + EPSILON)
    padded = jnp.concatenate([state[..., grid_x - HALO:], state, state[..., :HALO]], axis=3)
    coef_global = jnp.arange(coef_count, dtype=jnp.int32)

    def one_window(window_index):
        segment = lax.dynamic_slice_in_dim(padded, (window_index * X_DEV).astype(jnp.int32), window, 3)
        spectra = jnp.dot(segment.reshape(-1, window), projection, precision=HIGHEST, preferred_element_type=jnp.float32)
        spectra = spectra.reshape(members, fields, coef_count, 2 * MODES)
        rhs = advance(spectra, MODES, coef_global, coef_count)
        solved = jnp.einsum('mij,efjm->efim', inverse, rhs, precision=HIGHEST)
        values = jnp.dot(solved.reshape(-1, MODES), back_table, precision=HIGHEST, preferred_element_type=jnp.float32)
        return values.reshape(members, fields, coef_count, X_DEV)
    pieces = lax.map(one_window, jnp.arange(N_GX, dtype=jnp.int32))
    updated = jnp.moveaxis(pieces, 0, 3).reshape(members, fields, coef_count, grid_x) * renorm[:, None, None, None]
    chosen = jnp.stack([updated[:, 0], updated[:, 2]], axis=1)
    wall_stress = jnp.einsum('wk,eckx->ewcx', wall_weights(coef_global, coef_count), chosen, precision=HIGHEST)
    return (updated, wall_stress)
```

```python
import functools

import jax
import jax.numpy as jnp
import numpy as np
from jax import lax
from jax.experimental import pallas as pl
from jax.experimental.pallas import tpu as pltpu
from jax.sharding import PartitionSpec as P

MODES = 128
HALO = 64

EPSILON = 1e-06
TIME_STEP = 0.5
MEAN_FLOW = 0.8
CORIOLIS = 0.6
STRATIFICATION = 0.9

LANES = 128
GROUP = 4
NT = (((1,), (1,)), ((), ()))


def window_tables(window, rim_width, points, mode_count):
    position = np.arange(window)
    mode_index = np.arange(mode_count)
    half_count = mode_count // 2
    is_cosine = mode_index <= half_count
    wave_index = np.where(is_cosine, mode_index, mode_index - half_count)
    product_index = position[:, None] * wave_index[None, :] % window
    phases = 2.0 * np.pi * product_index / window
    weights_norm = np.where(wave_index == 0, np.sqrt(1.0 / window), np.sqrt(2.0 / window))
    basis = np.where(is_cosine[None, :], np.cos(phases), np.sin(phases)) * weights_norm[None, :]
    wavenumber = 2.0 * np.pi * wave_index / window
    paired = wave_index[:, None] == wave_index[None, :]
    to_sine = is_cosine[:, None] & ~is_cosine[None, :] & paired
    to_cosine = ~is_cosine[:, None] & is_cosine[None, :] & paired
    derivative = np.where(to_sine, -wavenumber[:, None], 0.0) + np.where(
        to_cosine, wavenumber[:, None], 0.0
    )
    taper = 0.25 + 0.75 * np.sin(np.pi * (position + 0.5) / window) ** 2
    values = basis * taper[:, None]
    slopes = (basis @ derivative) * taper[:, None]
    back_table = (
        basis[rim_width : rim_width + points, :] / taper[rim_width : rim_width + points, None]
    ).T
    return values, slopes, back_table


def step_tables(values, slopes, rim, points):
    direct = values - TIME_STEP * MEAN_FLOW * slopes
    couplings = (
        (TIME_STEP * CORIOLIS, -TIME_STEP * CORIOLIS),
        (TIME_STEP, -TIME_STEP * STRATIFICATION),
    )
    tables = []
    for to_first, to_second in couplings:
        first = (direct, to_first * values)
        second = (to_second * values, direct)
        rows = []
        for part in (first, second):
            pieces = []
            for begin, end in ((rim, rim + points), (0, rim), (rim + points, points + 2 * rim)):
                pieces += [part[0][begin:end].T, part[1][begin:end].T]
            rows.append(np.concatenate(pieces, axis=1))
        tables.append(np.concatenate(rows, axis=0))
    return np.stack(tables)


def split_table(table):
    table = np.asarray(table, np.float32)
    high = table.astype(jnp.bfloat16)
    low = (table - high.astype(np.float32)).astype(jnp.bfloat16)
    return jnp.asarray(high), jnp.asarray(low)


def split(x):
    high = x.astype(jnp.bfloat16)
    low = (x - high.astype(jnp.float32)).astype(jnp.bfloat16)
    return high, low


def dot(a, b, dims):
    return lax.dot_general(a, b, dims, preferred_element_type=jnp.float32)


def left_lanes(shape):
    return lax.broadcasted_iota(jnp.int32, shape, len(shape) - 1) < LANES // 2


def swap(x):
    return pltpu.roll(x, LANES // 2, len(x.shape) - 1)


def pack_kernel(state_ref, last_ref, first_ref, sums_ref):
    rows = state_ref.shape[2]
    left = left_lanes((rows, LANES))
    totals = []
    for e in range(GROUP):
        acc = jnp.zeros((rows, LANES), jnp.float32)
        for p in range(2):
            a = state_ref[e, p]
            b = state_ref[e, p + 2]
            acc += a * a + b * b
            last_ref[e, p] = jnp.where(left, swap(a), b)
            first_ref[e, p] = jnp.where(left, a, swap(b))
        totals.append(jnp.sum(acc))
    half = left_lanes((4, LANES))
    for q in range(GROUP // 2):
        sums_ref[4 * q : 4 * q + 4] = jnp.where(half, totals[2 * q], totals[2 * q + 1])


def project_kernel(state_ref, before_ref, after_ref, high_ref, low_ref, mask_ref, sums_ref, out_ref):
    parts, slots, rows, _ = out_ref.shape
    coef = state_ref.shape[2]
    count = (slots - 1) * parts
    flat = out_ref.reshape(parts * slots * rows, LANES)
    mask = mask_ref[...]
    for p in range(2):
        x = jnp.concatenate(
            [
                state_ref[:, p].reshape(GROUP * coef, LANES),
                state_ref[:, p + 2].reshape(GROUP * coef, LANES),
                before_ref[:, p].reshape(GROUP * coef, LANES),
                after_ref[:, p].reshape(GROUP * coef, LANES),
            ],
            axis=1,
        )
        x_high, x_low = split(x)
        w_high = high_ref[p]
        w_low = low_ref[p]
        t = dot(w_high, x_high, NT) + (dot(w_high, x_low, NT) + dot(w_low, x_high, NT))
        t = t * mask
        for f in range(2):
            for q in range(GROUP // 2):
                row = 4 * q + p + 2 * f
                for k in range(parts):
                    first = f * count + k * (slots - 1)
                    flat[pl.ds(k * slots * rows + row, slots - 1, stride=rows), :] = t[
                        first : first + slots - 1, q * LANES : (q + 1) * LANES
                    ]
    for k in range(parts):
        out_ref[k, slots - 1] = sums_ref[...]


def solve_kernel(total, recv_ref, inverse_ref, wall_ref, out_ref, scale_ref, wall_sums):
    step = pl.program_id(0)
    parts, slots, rows, _ = recv_ref.shape
    per_step = inverse_ref.shape[0]
    left = left_lanes((rows, LANES))

    @pl.when(step == 0)
    def _():
        n = recv_ref[0, slots - 1]
        for s in range(1, parts):
            n = n + recv_ref[s, slots - 1]
        scale_ref[...] = lax.rsqrt(n / total + EPSILON)
        wall_sums[...] = jnp.zeros_like(wall_sums)

    scale = scale_ref[...]
    lane = lax.broadcasted_iota(jnp.int32, (rows, LANES), 1)
    sums = wall_sums[...]
    for i in range(per_step):
        m = step * per_step + i
        t = [recv_ref[s, m] * scale for s in range(parts)]
        even, odd = [], []
        for s in range(0, parts, 2):
            even.append(jnp.where(left, t[s], swap(t[s + 1])))
            odd.append(jnp.where(left, swap(t[s]), t[s + 1]))
        r = jnp.concatenate(
            [jnp.concatenate(even, axis=1), jnp.concatenate(odd, axis=1)], axis=0
        )
        r_high, r_low = split(r)
        v_high, v_low = split(inverse_ref[i])
        both = dot(jnp.concatenate([r_high, r_low], axis=0), v_high, NT)
        o = both[: 2 * rows] + (both[2 * rows :] + dot(r_high, v_low, NT))
        for s in range(0, parts, 2):
            a = o[:rows, s * 64 : s * 64 + LANES]
            b = o[rows:, s * 64 : s * 64 + LANES]
            out_ref[s, m] = jnp.where(left, a, swap(b))
            out_ref[s + 1, m] = jnp.where(left, swap(a), b)
        for w in range(2):
            q = jnp.sum(o * wall_ref[w : w + 1, :], axis=1, keepdims=True)
            for e in range(2):
                at = e * 2 * (slots - 1) + w * (slots - 1) + m
                sums = jnp.where(lane == at, q[e * rows : (e + 1) * rows], sums)
    wall_sums[...] = sums

    @pl.when(step == pl.num_programs(0) - 1)
    def _():
        for k in range(parts):
            out_ref[k, slots - 1] = wall_sums[...]


def back_kernel(recv_ref, high_ref, low_ref, out_ref, wall_ref):
    parts, slots, rows, _ = recv_ref.shape
    coef = out_ref.shape[2]
    width = slots - 1
    flat = recv_ref.reshape(parts * slots * rows, LANES)
    b_high = high_ref[...]
    b_low = low_ref[...]
    for r in range(rows):
        q, f = r // 4, r % 4
        s = jnp.concatenate(
            [flat[pl.ds(k * slots * rows + r, width, stride=rows), :] for k in range(parts)],
            axis=0,
        )
        s = s.T
        s_high, s_low = split(s)
        dims = (((1,), (0,)), ((), ()))
        o = dot(s_high, b_high, dims) + (dot(s_high, b_low, dims) + dot(s_low, b_high, dims))
        for e in range(2):
            out_ref[2 * q + e, f] = o[e * coef : (e + 1) * coef]
    lane = lax.broadcasted_iota(jnp.int32, (rows, LANES), 1)
    for e in range(2):
        for w in range(2):
            g = jnp.zeros((rows, LANES), jnp.float32)
            for k in range(parts):
                tile = recv_ref[k, slots - 1]
                shift = (k * width - (e * 2 + w) * width) % LANES
                tile = pltpu.roll(tile, shift, 1) if shift else tile
                g = jnp.where((lane >= k * width) & (lane < (k + 1) * width), tile, g)
            g_high, g_low = split(g)
            dims = (((1,), (0,)), ((), ()))
            o = dot(g_high, b_high, dims) + (dot(g_high, b_low, dims) + dot(g_low, b_high, dims))
            for q in range(GROUP // 2):
                for c in range(2):
                    row = 4 * q + 2 * c
                    wall_ref[2 * q + e, w, c : c + 1] = o[row : row + 1]


def shifted(x, axis, by):
    n = lax.axis_size(axis)
    return lax.ppermute(x, axis, [(i, (i + by) % n) for i in range(n)])


def ring_sum(x, axis):
    n = lax.axis_size(axis)
    if n & (n - 1):
        return lax.psum(x, axis)
    hop = 1
    while hop < n:
        x = x + shifted(x, axis, hop)
        hop *= 2
    return x


def whole(shape):
    return pl.BlockSpec(shape, lambda *_: (0,) * len(shape))


def per_device(state, inverse):
    members, fields, coef, points = state.shape
    parts = lax.axis_size("gy")
    coef_count = coef * parts
    grid_x = points * lax.axis_size("gx")
    window = points + 2 * HALO
    mine = MODES // parts
    rows = members * fields * coef // LANES
    group_rows = GROUP * fields * coef // LANES
    groups = members // GROUP
    slots = mine + 1

    values, slopes, back_table = window_tables(window, HALO, points, MODES)
    step_high, step_low = split_table(step_tables(values, slopes, HALO, points))
    back_high, back_low = split_table(back_table)
    k = np.arange(coef_count)
    curvature = k * k / (coef_count * coef_count)
    wall = np.zeros((8, coef_count), np.float32)
    wall[0] = curvature
    wall[1] = np.where(k % 2 == 0, -1.0, 1.0) * curvature
    wall = jnp.asarray(wall)

    last, first, sums = pl.pallas_call(
        pack_kernel,
        grid=(groups,),
        in_specs=[pl.BlockSpec((GROUP, fields, coef, points), lambda g: (g, 0, 0, 0))],
        out_specs=[
            pl.BlockSpec((GROUP, 2, coef, LANES), lambda g: (g, 0, 0, 0)),
            pl.BlockSpec((GROUP, 2, coef, LANES), lambda g: (g, 0, 0, 0)),
            pl.BlockSpec((group_rows, LANES), lambda g: (g, 0)),
        ],
        out_shape=[
            jax.ShapeDtypeStruct((members, 2, coef, LANES), jnp.float32),
            jax.ShapeDtypeStruct((members, 2, coef, LANES), jnp.float32),
            jax.ShapeDtypeStruct((rows, LANES), jnp.float32),
        ],
        name="pack",
    )(state)
    before = shifted(last, "gx", 1)
    after = shifted(first, "gx", -1)
    sums = ring_sum(sums, "gx")

    coef_global = lax.axis_index("gy") * coef + jnp.arange(coef, dtype=jnp.int32)
    keep = (coef_global < coef_count - 2).astype(jnp.float32)
    mask = jnp.tile(keep, GROUP)[None, :]

    sent = pl.pallas_call(
        project_kernel,
        grid=(groups,),
        in_specs=[
            pl.BlockSpec((GROUP, fields, coef, points), lambda g: (g, 0, 0, 0)),
            pl.BlockSpec((GROUP, 2, coef, LANES), lambda g: (g, 0, 0, 0)),
            pl.BlockSpec((GROUP, 2, coef, LANES), lambda g: (g, 0, 0, 0)),
            whole(step_high.shape),
            whole(step_low.shape),
            whole(mask.shape),
            pl.BlockSpec((group_rows, LANES), lambda g: (g, 0)),
        ],
        out_specs=pl.BlockSpec((parts, slots, group_rows, LANES), lambda g: (0, 0, g, 0)),
        out_shape=jax.ShapeDtypeStruct((parts, slots, rows, LANES), jnp.float32),
        name="project",
    )(state, before, after, step_high, step_low, mask, sums)
    got = lax.all_to_all(sent, "gy", split_axis=0, concat_axis=0, tiled=True)

    per_step = 4
    solved = pl.pallas_call(
        functools.partial(solve_kernel, float(fields * coef_count * grid_x)),
        grid=(mine // per_step,),
        in_specs=[
            whole(got.shape),
            pl.BlockSpec((per_step, coef_count, coef_count), lambda i: (i, 0, 0)),
            whole(wall.shape),
        ],
        out_specs=whole(got.shape),
        out_shape=jax.ShapeDtypeStruct(got.shape, jnp.float32),
        scratch_shapes=[
            pltpu.VMEM((rows, LANES), jnp.float32),
            pltpu.VMEM((rows, LANES), jnp.float32),
        ],
        name="solve",
    )(got, inverse, wall)
    returned = lax.all_to_all(solved, "gy", split_axis=0, concat_axis=0, tiled=True)

    return pl.pallas_call(
        back_kernel,
        grid=(groups,),
        in_specs=[
            pl.BlockSpec((parts, slots, group_rows, LANES), lambda g: (0, 0, g, 0)),
            whole(back_high.shape),
            whole(back_low.shape),
        ],
        out_specs=[
            pl.BlockSpec((GROUP, fields, coef, points), lambda g: (g, 0, 0, 0)),
            pl.BlockSpec((GROUP, 2, 2, points), lambda g: (g, 0, 0, 0)),
        ],
        out_shape=[
            jax.ShapeDtypeStruct((members, fields, coef, points), jnp.float32),
            jax.ShapeDtypeStruct((members, 2, 2, points), jnp.float32),
        ],
        name="back",
    )(returned, back_high, back_low)


def solution(mesh):
    placed = (P(None, None, "gy", "gx"), P("gy", None, None))
    return jax.shard_map(
        per_device,
        mesh=mesh,
        in_specs=placed,
        out_specs=(P(None, None, "gy", "gx"), P(None, None, None, "gx")),
        check_vma=False,
    )
```

```python
import functools

import jax
import jax.numpy as jnp
import numpy as np
from jax import lax
from jax.experimental import pallas as pl
from jax.experimental.pallas import tpu as pltpu
from jax.sharding import PartitionSpec as P

MODES = 128
HALO = 64

EPSILON = 1e-06
TIME_STEP = 0.5
MEAN_FLOW = 0.8
CORIOLIS = 0.6
STRATIFICATION = 0.9

LANES = 128
MIB = 1 << 20
GROUP = 4
NT = (((1,), (1,)), ((), ()))
NN = (((1,), (0,)), ((), ()))


def window_tables(window, rim_width, points, mode_count):
    position = np.arange(window)
    mode_index = np.arange(mode_count)
    half_count = mode_count // 2
    is_cosine = mode_index <= half_count
    wave_index = np.where(is_cosine, mode_index, mode_index - half_count)
    product_index = position[:, None] * wave_index[None, :] % window
    phases = 2.0 * np.pi * product_index / window
    weights_norm = np.where(wave_index == 0, np.sqrt(1.0 / window), np.sqrt(2.0 / window))
    basis = np.where(is_cosine[None, :], np.cos(phases), np.sin(phases)) * weights_norm[None, :]
    wavenumber = 2.0 * np.pi * wave_index / window
    paired = wave_index[:, None] == wave_index[None, :]
    to_sine = is_cosine[:, None] & ~is_cosine[None, :] & paired
    to_cosine = ~is_cosine[:, None] & is_cosine[None, :] & paired
    derivative = np.where(to_sine, -wavenumber[:, None], 0.0) + np.where(
        to_cosine, wavenumber[:, None], 0.0
    )
    taper = 0.25 + 0.75 * np.sin(np.pi * (position + 0.5) / window) ** 2
    values = basis * taper[:, None]
    slopes = (basis @ derivative) * taper[:, None]
    back_table = (
        basis[rim_width : rim_width + points, :] / taper[rim_width : rim_width + points, None]
    ).T
    return values, slopes, back_table


def step_tables(values, slopes, rim, points):
    direct = values - TIME_STEP * MEAN_FLOW * slopes
    couplings = (
        (TIME_STEP * CORIOLIS, -TIME_STEP * CORIOLIS),
        (TIME_STEP, -TIME_STEP * STRATIFICATION),
    )
    tables = []
    for to_first, to_second in couplings:
        first = (direct, to_first * values)
        second = (to_second * values, direct)
        rows = []
        for part in (first, second):
            pieces = []
            for begin, end in ((rim, rim + points), (0, rim), (rim + points, points + 2 * rim)):
                pieces += [part[0][begin:end].T, part[1][begin:end].T]
            rows.append(np.concatenate(pieces, axis=1))
        tables.append(np.concatenate(rows, axis=0))
    return np.stack(tables)


def split_table(table):
    table = np.asarray(table, np.float32)
    high = table.astype(jnp.bfloat16)
    low = (table - high.astype(np.float32)).astype(jnp.bfloat16)
    return jnp.asarray(high), jnp.asarray(low)


def split(x):
    high = x.astype(jnp.bfloat16)
    low = (x - high.astype(jnp.float32)).astype(jnp.bfloat16)
    return high, low


def dot(a, b, dims):
    return lax.dot_general(a, b, dims, preferred_element_type=jnp.float32)


def left_lanes(shape):
    return lax.broadcasted_iota(jnp.int32, shape, len(shape) - 1) < LANES // 2


def swap(x):
    return pltpu.roll(x, LANES // 2, len(x.shape) - 1)


def pack_kernel(state_ref, last_ref, first_ref, sums_ref):
    rows = state_ref.shape[2]
    left = left_lanes((rows, LANES))
    totals = []
    for e in range(GROUP):
        acc = jnp.zeros((rows, LANES), jnp.float32)
        for p in range(2):
            a = state_ref[e, p]
            b = state_ref[e, p + 2]
            acc += a * a + b * b
            last_ref[e, p] = jnp.where(left, swap(a), b)
            first_ref[e, p] = jnp.where(left, a, swap(b))
        totals.append(jnp.sum(acc))
    half = left_lanes((4, LANES))
    for q in range(GROUP // 2):
        sums_ref[4 * q : 4 * q + 4] = jnp.where(half, totals[2 * q], totals[2 * q + 1])


def split_kernel(inverse_ref, high_ref, low_ref):
    high_ref[...], low_ref[...] = split(inverse_ref[...])


def project_kernel(state_ref, before_ref, after_ref, high_ref, low_ref, mask_ref, out_ref):
    parts, slots, rows, _ = out_ref.shape
    coef = state_ref.shape[2]
    count = slots * parts
    flat = out_ref.reshape(parts * slots * rows, LANES)
    mask = mask_ref[...]
    for p in range(2):
        x = jnp.concatenate(
            [
                state_ref[:, p].reshape(GROUP * coef, LANES),
                state_ref[:, p + 2].reshape(GROUP * coef, LANES),
                before_ref[:, p].reshape(GROUP * coef, LANES),
                after_ref[:, p].reshape(GROUP * coef, LANES),
            ],
            axis=1,
        )
        x_high, x_low = split(x)
        w_high = high_ref[p]
        w_low = low_ref[p]
        t = dot(w_high, x_high, NT) + (dot(w_high, x_low, NT) + dot(w_low, x_high, NT))
        t = t * mask
        for f in range(2):
            for q in range(GROUP // 2):
                row = 4 * q + p + 2 * f
                flat[pl.ds(row, count, stride=rows), :] = t[
                    f * count : (f + 1) * count, q * LANES : (q + 1) * LANES
                ]


def solve_kernel(recv_ref, high_ref, low_ref, wall_ref, sums_ref, out_ref):
    parts, slots, rows, _ = recv_ref.shape
    left = left_lanes((rows, LANES))
    lane = lax.broadcasted_iota(jnp.int32, (rows, LANES), 1)
    sums = jnp.zeros((rows, LANES), jnp.float32)
    for m in range(slots):
        t = [recv_ref[s, m] for s in range(parts)]
        even, odd = [], []
        for s in range(0, parts, 2):
            even.append(jnp.where(left, t[s], swap(t[s + 1])))
            odd.append(jnp.where(left, swap(t[s]), t[s + 1]))
        r = jnp.concatenate(
            [jnp.concatenate(even, axis=1), jnp.concatenate(odd, axis=1)], axis=0
        )
        r_high, r_low = split(r)
        v_high = high_ref[m]
        v_low = low_ref[m]
        both = dot(jnp.concatenate([r_high, r_low], axis=0), v_high, NT)
        o = both[: 2 * rows] + (both[2 * rows :] + dot(r_high, v_low, NT))
        for s in range(0, parts, 2):
            a = o[:rows, s * 64 : s * 64 + LANES]
            b = o[rows:, s * 64 : s * 64 + LANES]
            out_ref[s, m] = jnp.where(left, a, swap(b))
            out_ref[s + 1, m] = jnp.where(left, swap(a), b)
        for w in range(2):
            q = jnp.sum(o * wall_ref[w : w + 1, :], axis=1, keepdims=True)
            for e in range(2):
                at = e * 2 * slots + w * slots + m
                sums = jnp.where(lane == at, q[e * rows : (e + 1) * rows], sums)
    for k in range(parts):
        out_ref[k, slots] = sums
        out_ref[k, slots + 1] = sums_ref[...]


def back_kernel(total, recv_ref, high_ref, low_ref, *refs):
    out_ref, wall_ref = refs[-2:]
    parts, slots, rows, _ = recv_ref.shape
    coef = out_ref.shape[2]
    width = slots - 2
    flat = recv_ref.reshape(parts * slots * rows, LANES)
    b_high = high_ref[...]
    b_low = low_ref[...]
    n = recv_ref[0, slots - 1]
    for k in range(1, parts):
        n = n + recv_ref[k, slots - 1]
    scale = lax.rsqrt(n / total + EPSILON)
    for r in range(rows):
        q, f = r // 4, r % 4
        s = jnp.concatenate(
            [flat[pl.ds(k * slots * rows + r, width, stride=rows), :] for k in range(parts)],
            axis=0,
        )
        s = (s * scale[r : r + 1]).T
        s_high, s_low = split(s)
        o = dot(s_high, b_high, NN) + (dot(s_high, b_low, NN) + dot(s_low, b_high, NN))
        for e in range(2):
            out_ref[2 * q + e, f] = o[e * coef : (e + 1) * coef]
    lane = lax.broadcasted_iota(jnp.int32, (rows, LANES), 1)
    tiles = [recv_ref[k, slots - 2] * scale for k in range(parts)]
    for e in range(2):
        for w in range(2):
            g = jnp.zeros((rows, LANES), jnp.float32)
            for k in range(parts):
                shift = (k * width - (e * 2 + w) * width) % LANES
                tile = pltpu.roll(tiles[k], shift, 1) if shift else tiles[k]
                g = jnp.where((lane >= k * width) & (lane < (k + 1) * width), tile, g)
            g_high, g_low = split(g)
            o = dot(g_high, b_high, NN) + (dot(g_high, b_low, NN) + dot(g_low, b_high, NN))
            for q in range(GROUP // 2):
                for c in range(2):
                    row = 4 * q + 2 * c
                    wall_ref[2 * q + e, w, c : c + 1] = o[row : row + 1]


def shifted(x, axis, by):
    n = lax.axis_size(axis)
    return lax.ppermute(x, axis, [(i, (i + by) % n) for i in range(n)])


def ring_sum(x, axis):
    n = lax.axis_size(axis)
    if n & (n - 1):
        return lax.psum(x, axis)
    hop = 1
    while hop < n:
        x = x + shifted(x, axis, hop)
        hop *= 2
    return x


def whole(shape):
    return pl.BlockSpec(shape, lambda *_: (0,) * len(shape))


def per_device(state, inverse):
    members, fields, coef, points = state.shape
    parts = lax.axis_size("gy")
    coef_count = coef * parts
    grid_x = points * lax.axis_size("gx")
    window = points + 2 * HALO
    mine = MODES // parts
    group_rows = GROUP * fields * coef // LANES
    groups = members // GROUP

    values, slopes, back_table = window_tables(window, HALO, points, MODES)
    step_high, step_low = split_table(step_tables(values, slopes, HALO, points))
    back_high, back_low = split_table(back_table)
    k = np.arange(coef_count)
    curvature = k * k / (coef_count * coef_count)
    wall = np.zeros((8, coef_count), np.float32)
    wall[0] = curvature
    wall[1] = np.where(k % 2 == 0, -1.0, 1.0) * curvature
    wall = jnp.asarray(wall)

    coef_global = lax.axis_index("gy") * coef + jnp.arange(coef, dtype=jnp.int32)
    keep = (coef_global < coef_count - 2).astype(jnp.float32)
    mask = jnp.tile(keep, GROUP)[None, :]

    def grouped(g, shape):
        return pl.BlockSpec((GROUP,) + shape, lambda i: (g,) + (0,) * len(shape))

    def call(kernel, name, vmem, flops, moved, **kwargs):
        return pl.pallas_call(
            kernel,
            grid=(1,),
            name=name,
            compiler_params=pltpu.CompilerParams(vmem_limit_bytes=vmem * MIB),
            cost_estimate=pl.CostEstimate(flops=flops, bytes_accessed=moved, transcendentals=0),
            **kwargs,
        )

    block = (fields, coef, points)
    halo = (GROUP, 2, coef, LANES)
    halo_bytes = 4 * int(np.prod(halo))
    small = (group_rows, LANES)
    sent_shape = (parts, mine, group_rows, LANES)
    back_shape = (parts, mine + 2, group_rows, LANES)

    packed = []
    for g in range(groups):
        packed.append(
            call(
                pack_kernel,
                f"pack{g}",
                6,
                10**6,
                4 * halo_bytes,
                in_specs=[grouped(g, block)],
                out_specs=[whole(halo), whole(halo), whole(small)],
                out_shape=[
                    jax.ShapeDtypeStruct(halo, jnp.float32),
                    jax.ShapeDtypeStruct(halo, jnp.float32),
                    jax.ShapeDtypeStruct(small, jnp.float32),
                ],
            )(state)
        )
    halos = [(shifted(p[0], "gx", 1), shifted(p[1], "gx", -1)) for p in packed]
    sums = ring_sum(jnp.concatenate([p[2] for p in packed], axis=0), "gx")

    per_step = 4
    split_shape = (per_step, coef_count, coef_count)
    inverse_high, inverse_low = pl.pallas_call(
        split_kernel,
        grid=(mine // per_step,),
        in_specs=[pl.BlockSpec(split_shape, lambda i: (i, 0, 0))],
        out_specs=[pl.BlockSpec(split_shape, lambda i: (i, 0, 0))] * 2,
        out_shape=[jax.ShapeDtypeStruct(inverse.shape, jnp.bfloat16)] * 2,
        name="split",
        compiler_params=pltpu.CompilerParams(vmem_limit_bytes=8 * MIB),
        cost_estimate=pl.CostEstimate(
            flops=10**7, bytes_accessed=8 * mine * coef_count**2, transcendentals=0
        ),
    )(inverse)

    outputs = []
    for g in range(groups):
        sent = call(
            project_kernel,
            f"project{g}",
            8,
            2 * 3 * 2 * 256 * 512 * GROUP * coef,
            6 * halo_bytes,
            in_specs=[
                grouped(g, block),
                whole(halo),
                whole(halo),
                whole(step_high.shape),
                whole(step_low.shape),
                whole(mask.shape),
            ],
            out_specs=whole(sent_shape),
            out_shape=jax.ShapeDtypeStruct(sent_shape, jnp.float32),
        )(state, *halos[g], step_high, step_low, mask)
        got = lax.all_to_all(sent, "gy", split_axis=0, concat_axis=0, tiled=True)
        solved = call(
            solve_kernel,
            f"solve{g}",
            24,
            2 * 3 * mine * coef_count**2 * 256,
            4 * mine * coef_count**2,
            in_specs=[
                whole(sent_shape),
                whole(inverse.shape),
                whole(inverse.shape),
                whole(wall.shape),
                pl.BlockSpec(small, lambda i: (g, 0)),
            ],
            out_specs=whole(back_shape),
            out_shape=jax.ShapeDtypeStruct(back_shape, jnp.float32),
        )(got, inverse_high, inverse_low, wall, sums)
        returned = lax.all_to_all(solved, "gy", split_axis=0, concat_axis=0, tiled=True)
        outputs = call(
            functools.partial(back_kernel, float(fields * coef_count * grid_x)),
            f"back{g}",
            8,
            2 * 3 * 128 * 128 * GROUP * fields * coef,
            4 * halo_bytes,
            in_specs=[whole(back_shape), whole(back_high.shape), whole(back_low.shape)]
            + [pl.BlockSpec(memory_space=pl.ANY)] * len(outputs),
            out_specs=[grouped(g, block), grouped(g, (2, 2, points))],
            out_shape=[
                jax.ShapeDtypeStruct(state.shape, jnp.float32),
                jax.ShapeDtypeStruct((members, 2, 2, points), jnp.float32),
            ],
            input_output_aliases={3 + i: i for i in range(len(outputs))},
        )(returned, back_high, back_low, *outputs)
    return tuple(outputs)


def solution(mesh):
    placed = (P(None, None, "gy", "gx"), P("gy", None, None))
    return jax.shard_map(
        per_device,
        mesh=mesh,
        in_specs=placed,
        out_specs=(P(None, None, "gy", "gx"), P(None, None, None, "gx")),
        check_vma=False,
    )
```

```python
import functools

import jax
import jax.numpy as jnp
import numpy as np
from jax import lax
from jax.experimental import pallas as pl
from jax.experimental.pallas import tpu as pltpu
from jax.sharding import PartitionSpec as P


MODES = 128
HALO = 64

EPSILON = 1e-06
TIME_STEP = 0.5
MEAN_FLOW = 0.8
CORIOLIS = 0.6
STRATIFICATION = 0.9

LANES = 128
MIB = 1 << 20
GROUP = 4
VMEM = pl.BlockSpec(memory_space=pltpu.VMEM)
NT = (((1,), (1,)), ((), ()))
NN = (((1,), (0,)), ((), ()))


def window_tables(window, rim_width, points, mode_count):
    position = np.arange(window)
    mode_index = np.arange(mode_count)
    half_count = mode_count // 2
    is_cosine = mode_index <= half_count
    wave_index = np.where(is_cosine, mode_index, mode_index - half_count)
    product_index = position[:, None] * wave_index[None, :] % window
    phases = 2.0 * np.pi * product_index / window
    weights_norm = np.where(wave_index == 0, np.sqrt(1.0 / window), np.sqrt(2.0 / window))
    basis = np.where(is_cosine[None, :], np.cos(phases), np.sin(phases)) * weights_norm[None, :]
    wavenumber = 2.0 * np.pi * wave_index / window
    paired = wave_index[:, None] == wave_index[None, :]
    to_sine = is_cosine[:, None] & ~is_cosine[None, :] & paired
    to_cosine = ~is_cosine[:, None] & is_cosine[None, :] & paired
    derivative = np.where(to_sine, -wavenumber[:, None], 0.0) + np.where(
        to_cosine, wavenumber[:, None], 0.0
    )
    taper = 0.25 + 0.75 * np.sin(np.pi * (position + 0.5) / window) ** 2
    values = basis * taper[:, None]
    slopes = (basis @ derivative) * taper[:, None]
    back_table = (
        basis[rim_width : rim_width + points, :] / taper[rim_width : rim_width + points, None]
    ).T
    return values, slopes, back_table


def step_tables(values, slopes, rim, points):
    direct = values - TIME_STEP * MEAN_FLOW * slopes
    couplings = (
        (TIME_STEP * CORIOLIS, -TIME_STEP * CORIOLIS),
        (TIME_STEP, -TIME_STEP * STRATIFICATION),
    )
    tables = []
    for to_first, to_second in couplings:
        first = (direct, to_first * values)
        second = (to_second * values, direct)
        rows = []
        for part in (first, second):
            pieces = []
            for begin, end in ((rim, rim + points), (0, rim), (rim + points, points + 2 * rim)):
                pieces += [part[0][begin:end].T, part[1][begin:end].T]
            rows.append(np.concatenate(pieces, axis=1))
        tables.append(np.concatenate(rows, axis=0))
    return np.stack(tables)


def split_table(table):
    table = np.asarray(table, np.float32)
    high = table.astype(jnp.bfloat16)
    low = (table - high.astype(np.float32)).astype(jnp.bfloat16)
    return jnp.asarray(high), jnp.asarray(low)


def split(x):
    high = x.astype(jnp.bfloat16)
    low = (x - high.astype(jnp.float32)).astype(jnp.bfloat16)
    return high, low


def dot(a, b, dims):
    return lax.dot_general(a, b, dims, preferred_element_type=jnp.float32)


def left_lanes(shape):
    return lax.broadcasted_iota(jnp.int32, shape, len(shape) - 1) < LANES // 2


def swap(x):
    return pltpu.roll(x, LANES // 2, len(x.shape) - 1)


def pack_kernel(base, state_ref, last_ref, first_ref, sums_ref):
    rows = state_ref.shape[2]
    left = left_lanes((rows, LANES))
    totals = []
    for e in range(GROUP):
        acc = jnp.zeros((rows, LANES), jnp.float32)
        for p in range(2):
            a = state_ref[base + e, p]
            b = state_ref[base + e, p + 2]
            acc += a * a + b * b
            last_ref[e, p] = jnp.where(left, swap(a), b)
            first_ref[e, p] = jnp.where(left, a, swap(b))
        totals.append(jnp.sum(acc))
    half = left_lanes((4, LANES))
    for q in range(GROUP // 2):
        sums_ref[4 * q : 4 * q + 4] = jnp.where(half, totals[2 * q], totals[2 * q + 1])


def peers(parts):
    me = lax.axis_index("gy")
    return [jnp.bitwise_xor(me, d) for d in range(parts)]


def reorder_lanes(x):
    me = lax.axis_index("gy")
    far = jnp.bitwise_and(me, 2) != 0
    near = jnp.bitwise_and(me, 1) != 0
    a, b = x[..., :LANES], x[..., LANES:]
    a, b = jnp.where(far, b, a), jnp.where(far, a, b)
    return jnp.where(near, swap(a), a), jnp.where(near, swap(b), b)


def split_kernel(inverse_ref, high_ref, low_ref):
    coef_count = inverse_ref.shape[1]
    coef = LANES // 2
    for d, peer in enumerate(peers(coef_count // coef)):
        rows = pl.ds(pl.multiple_of(peer * coef, coef), coef)
        for h, x in enumerate(reorder_lanes(inverse_ref[:, rows, :])):
            at = (slice(None), slice(d * coef, (d + 1) * coef), slice(h * LANES, (h + 1) * LANES))
            high_ref[at], low_ref[at] = split(x)


def project_kernel(base, state_ref, before_ref, after_ref, high_ref, low_ref, mask_ref, *out_refs):
    parts = len(out_refs)
    slots, rows, _ = out_refs[0].shape
    coef = state_ref.shape[2]
    count = slots * parts
    mask = mask_ref[...]
    where = [pl.multiple_of(peer * slots, slots) for peer in peers(parts)]
    for p in range(2):
        x = jnp.concatenate(
            [
                state_ref[base : base + GROUP, p].reshape(GROUP * coef, LANES),
                state_ref[base : base + GROUP, p + 2].reshape(GROUP * coef, LANES),
                before_ref[:, p].reshape(GROUP * coef, LANES),
                after_ref[:, p].reshape(GROUP * coef, LANES),
            ],
            axis=1,
        )
        x_high, x_low = split(x)
        w_high, w_low = [
            jnp.concatenate(
                [ref[p, pl.ds(f * count + at, slots), :] for f in range(2) for at in where], axis=0
            )
            for ref in (high_ref, low_ref)
        ]
        t = dot(w_high, x_high, NT) + (dot(w_high, x_low, NT) + dot(w_low, x_high, NT))
        t = t * mask
        for d in range(parts):
            flat = out_refs[d].reshape(slots * rows, LANES)
            for f in range(2):
                first = f * count + d * slots
                for q in range(GROUP // 2):
                    flat[pl.ds(4 * q + p + 2 * f, slots, stride=rows), :] = t[
                        first : first + slots, q * LANES : (q + 1) * LANES
                    ]


def solve_kernel(base, parts, *refs):
    recv_refs = refs[:parts]
    high_ref, low_ref, wall_ref, sums_ref = refs[parts : parts + 4]
    out_refs = refs[parts + 4 :]
    slots, rows, _ = recv_refs[0].shape
    left = left_lanes((rows, LANES))
    lane = lax.broadcasted_iota(jnp.int32, (rows, LANES), 1)
    wall = jnp.concatenate(reorder_lanes(wall_ref[...]), axis=1)
    sums = jnp.zeros((rows, LANES), jnp.float32)
    for m in range(slots):
        t = [ref[m] for ref in recv_refs]
        even, odd = [], []
        for d in range(0, parts, 2):
            even.append(jnp.where(left, t[d], swap(t[d + 1])))
            odd.append(jnp.where(left, swap(t[d]), t[d + 1]))
        r = jnp.concatenate(
            [jnp.concatenate(even, axis=1), jnp.concatenate(odd, axis=1)], axis=0
        )
        r_high, r_low = split(r)
        v_high = high_ref[m]
        v_low = low_ref[m]
        both = dot(jnp.concatenate([r_high, r_low], axis=0), v_high, NT)
        o = both[: 2 * rows] + (both[2 * rows :] + dot(r_high, v_low, NT))
        for d in range(0, parts, 2):
            a = o[:rows, d * 64 : d * 64 + LANES]
            b = o[rows:, d * 64 : d * 64 + LANES]
            out_refs[d][m] = jnp.where(left, a, swap(b))
            out_refs[d + 1][m] = jnp.where(left, swap(a), b)
        for w in range(2):
            q = jnp.sum(o * wall[w : w + 1], axis=1, keepdims=True)
            for e in range(2):
                at = e * 2 * slots + w * slots + m
                sums = jnp.where(lane == at, q[e * rows : (e + 1) * rows], sums)
    for ref in out_refs:
        ref[slots] = sums
        ref[slots + 1] = sums_ref[base : base + rows]


def back_kernel(total, parts, *refs):
    recv_refs = refs[:parts]
    high_ref, low_ref = refs[parts : parts + 2]
    out_ref, wall_ref = refs[-2:]
    slots, rows, _ = recv_refs[0].shape
    coef = out_ref.shape[2]
    width = slots - 2
    where = [pl.multiple_of(peer * width, width) for peer in peers(parts)]
    b_high, b_low = [
        jnp.concatenate([ref[pl.ds(at, width), :] for at in where], axis=0)
        for ref in (high_ref, low_ref)
    ]
    n = [ref[slots - 1] for ref in recv_refs]
    me = lax.axis_index("gy")
    near = jnp.bitwise_and(me, 1) != 0
    far = jnp.bitwise_and(me, 2) != 0
    n = [jnp.where(near, n[d ^ 1], n[d]) for d in range(parts)]
    n = [jnp.where(far, n[d ^ 2], n[d]) for d in range(parts)]
    scale = lax.rsqrt(sum(n[1:], n[0]) / total + EPSILON)
    for r in range(rows):
        q, f = r // 4, r % 4
        s = jnp.concatenate(
            [
                ref.reshape(slots * rows, LANES)[pl.ds(r, width, stride=rows), :]
                for ref in recv_refs
            ],
            axis=0,
        )
        s = (s * scale[r : r + 1]).T
        s_high, s_low = split(s)
        o = dot(s_high, b_high, NN) + (dot(s_high, b_low, NN) + dot(s_low, b_high, NN))
        for e in range(2):
            out_ref[2 * q + e, f] = o[e * coef : (e + 1) * coef]
    lane = lax.broadcasted_iota(jnp.int32, (rows, LANES), 1)
    tiles = [ref[slots - 2] for ref in recv_refs]
    tiles = [jnp.where(near, tiles[d ^ 1], tiles[d]) for d in range(parts)]
    tiles = [jnp.where(far, tiles[d ^ 2], tiles[d]) * scale for d in range(parts)]
    b_high = high_ref[...]
    b_low = low_ref[...]
    for e in range(2):
        for w in range(2):
            g = jnp.zeros((rows, LANES), jnp.float32)
            for k in range(parts):
                shift = (k * width - (e * 2 + w) * width) % LANES
                tile = pltpu.roll(tiles[k], shift, 1) if shift else tiles[k]
                g = jnp.where((lane >= k * width) & (lane < (k + 1) * width), tile, g)
            g_high, g_low = split(g)
            o = dot(g_high, b_high, NN) + (dot(g_high, b_low, NN) + dot(g_low, b_high, NN))
            for q in range(GROUP // 2):
                for c in range(2):
                    row = 4 * q + 2 * c
                    wall_ref[2 * q + e, w, c : c + 1] = o[row : row + 1]


def shifted(x, axis, by):
    n = lax.axis_size(axis)
    return lax.ppermute(x, axis, [(i, (i + by) % n) for i in range(n)])


def exchanged(pieces, axis):
    n = lax.axis_size(axis)
    got = list(pieces)
    for d in range(n - 1, 0, -1):
        got[d] = lax.ppermute(pieces[d], axis, [(i, i ^ d) for i in range(n)])
    return got


def ring_sum(x, axis):
    n = lax.axis_size(axis)
    if n & (n - 1):
        return lax.psum(x, axis)
    hop = 1
    while hop < n:
        other = shifted(x, axis, hop)
        x = x + other
        hop *= 2
    return x


def per_device(state, inverse):
    members, fields, coef, points = state.shape
    parts = lax.axis_size("gy")
    coef_count = coef * parts
    grid_x = points * lax.axis_size("gx")
    window = points + 2 * HALO
    mine = MODES // parts
    group_rows = GROUP * fields * coef // LANES
    groups = members // GROUP

    values, slopes, back_table = window_tables(window, HALO, points, MODES)
    step_high, step_low = split_table(step_tables(values, slopes, HALO, points))
    back_high, back_low = split_table(back_table)
    k = np.arange(coef_count)
    curvature = k * k / (coef_count * coef_count)
    wall = np.zeros((8, coef_count), np.float32)
    wall[0] = curvature
    wall[1] = np.where(k % 2 == 0, -1.0, 1.0) * curvature
    wall = jnp.asarray(wall)

    coef_global = lax.axis_index("gy") * coef + jnp.arange(coef, dtype=jnp.int32)
    keep = (coef_global < coef_count - 2).astype(jnp.float32)
    mask = jnp.tile(keep, GROUP)[None, :]

    def grouped(g, shape):
        return pl.BlockSpec((GROUP,) + shape, lambda i: (g,) + (0,) * len(shape))

    def call(kernel, vmem, flops, moved, **kwargs):
        return pl.pallas_call(
            kernel,
            compiler_params=pltpu.CompilerParams(vmem_limit_bytes=vmem * MIB),
            cost_estimate=pl.CostEstimate(flops=flops, bytes_accessed=moved, transcendentals=0),
            **kwargs,
        )

    block = (fields, coef, points)
    halo = (GROUP, 2, coef, LANES)
    halo_bytes = 4 * int(np.prod(halo))
    small = (group_rows, LANES)
    sent_shape = (mine, group_rows, LANES)
    back_shape = (mine + 2, group_rows, LANES)

    packed = []
    for g in range(groups):
        packed.append(
            call(
                functools.partial(pack_kernel, g * GROUP),
                6,
                10**6,
                4 * halo_bytes,
                in_specs=[VMEM],
                out_specs=[VMEM] * 3,
                out_shape=[
                    jax.ShapeDtypeStruct(halo, jnp.float32),
                    jax.ShapeDtypeStruct(halo, jnp.float32),
                    jax.ShapeDtypeStruct(small, jnp.float32),
                ],
            )(state)
        )
    halos = []
    for last, first, _ in packed:
        before = shifted(last, "gx", 1)
        after = shifted(first, "gx", -1)
        halos.append((before, after))
    sums = ring_sum(jnp.concatenate([p[2] for p in packed], axis=0), "gx")

    per_step = 4
    split_shape = (per_step, coef_count, coef_count)
    inverse_high, inverse_low = pl.pallas_call(
        split_kernel,
        grid=(mine // per_step,),
        in_specs=[pl.BlockSpec(split_shape, lambda i: (i, 0, 0))],
        out_specs=[pl.BlockSpec(split_shape, lambda i: (i, 0, 0))] * 2,
        out_shape=[jax.ShapeDtypeStruct(inverse.shape, jnp.bfloat16)] * 2,
        name="split",
        compiler_params=pltpu.CompilerParams(vmem_limit_bytes=8 * MIB),
        cost_estimate=pl.CostEstimate(
            flops=10**7, bytes_accessed=8 * mine * coef_count**2, transcendentals=0
        ),
    )(inverse)

    outputs = []
    for g in range(groups):
        sent = call(
            functools.partial(project_kernel, g * GROUP),
            8,
            2 * 3 * 2 * 256 * 512 * GROUP * coef,
            6 * halo_bytes,
            in_specs=[VMEM] * 6,
            out_specs=[VMEM] * parts,
            out_shape=[jax.ShapeDtypeStruct(sent_shape, jnp.float32)] * parts,
        )(state, *halos[g], step_high, step_low, mask)
        got = exchanged(sent, "gy")
        solved = call(
            functools.partial(solve_kernel, g * group_rows, parts),
            24,
            2 * 3 * mine * coef_count**2 * 256,
            4 * mine * coef_count**2,
            in_specs=[VMEM] * (parts + 4),
            out_specs=[VMEM] * parts,
            out_shape=[jax.ShapeDtypeStruct(back_shape, jnp.float32)] * parts,
        )(*got, inverse_high, inverse_low, wall, sums)
        returned = exchanged(solved, "gy")
        outputs = call(
            functools.partial(back_kernel, float(fields * coef_count * grid_x), parts),
            8,
            2 * 3 * 128 * 128 * GROUP * fields * coef,
            4 * halo_bytes,
            grid=(1,),
            in_specs=[VMEM] * (parts + 2)
            + [pl.BlockSpec(memory_space=pl.ANY)] * len(outputs),
            out_specs=[grouped(g, block), grouped(g, (2, 2, points))],
            out_shape=[
                jax.ShapeDtypeStruct(state.shape, jnp.float32),
                jax.ShapeDtypeStruct((members, 2, 2, points), jnp.float32),
            ],
            input_output_aliases={parts + 2 + i: i for i in range(len(outputs))},
        )(*returned, back_high, back_low, *outputs)
    return tuple(outputs)


def solution(mesh):
    placed = (P(None, None, "gy", "gx"), P("gy", None, None))

    return jax.shard_map(
        per_device,
        mesh=mesh,
        in_specs=placed,
        out_specs=(P(None, None, "gy", "gx"), P(None, None, None, "gx")),
        check_vma=False,
    )
```

```python
import functools

import jax
import jax.numpy as jnp
import numpy as np
from jax import lax
from jax.experimental import pallas as pl
from jax.experimental.pallas import tpu as pltpu
from jax.sharding import PartitionSpec as P


MODES = 128
HALO = 64

EPSILON = 1e-06
TIME_STEP = 0.5
MEAN_FLOW = 0.8
CORIOLIS = 0.6
STRATIFICATION = 0.9

LANES = 128
MIB = 1 << 20
GROUP = 4
VMEM = pl.BlockSpec(memory_space=pltpu.VMEM)
NT = (((1,), (1,)), ((), ()))
NN = (((1,), (0,)), ((), ()))


def window_tables(window, rim_width, points, mode_count):
    position = np.arange(window)
    mode_index = np.arange(mode_count)
    half_count = mode_count // 2
    is_cosine = mode_index <= half_count
    wave_index = np.where(is_cosine, mode_index, mode_index - half_count)
    product_index = position[:, None] * wave_index[None, :] % window
    phases = 2.0 * np.pi * product_index / window
    weights_norm = np.where(wave_index == 0, np.sqrt(1.0 / window), np.sqrt(2.0 / window))
    basis = np.where(is_cosine[None, :], np.cos(phases), np.sin(phases)) * weights_norm[None, :]
    wavenumber = 2.0 * np.pi * wave_index / window
    paired = wave_index[:, None] == wave_index[None, :]
    to_sine = is_cosine[:, None] & ~is_cosine[None, :] & paired
    to_cosine = ~is_cosine[:, None] & is_cosine[None, :] & paired
    derivative = np.where(to_sine, -wavenumber[:, None], 0.0) + np.where(
        to_cosine, wavenumber[:, None], 0.0
    )
    taper = 0.25 + 0.75 * np.sin(np.pi * (position + 0.5) / window) ** 2
    values = basis * taper[:, None]
    slopes = (basis @ derivative) * taper[:, None]
    back_table = (
        basis[rim_width : rim_width + points, :] / taper[rim_width : rim_width + points, None]
    ).T
    return values, slopes, back_table


def step_tables(values, slopes, rim, points):
    direct = values - TIME_STEP * MEAN_FLOW * slopes
    couplings = (
        (TIME_STEP * CORIOLIS, -TIME_STEP * CORIOLIS),
        (TIME_STEP, -TIME_STEP * STRATIFICATION),
    )
    tables = []
    for to_first, to_second in couplings:
        first = (direct, to_first * values)
        second = (to_second * values, direct)
        rows = []
        for part in (first, second):
            pieces = []
            for begin, end in ((rim, rim + points), (0, rim), (rim + points, points + 2 * rim)):
                pieces += [part[0][begin:end].T, part[1][begin:end].T]
            rows.append(np.concatenate(pieces, axis=1))
        tables.append(np.concatenate(rows, axis=0))
    return np.stack(tables)


def split_table(table):
    table = np.asarray(table, np.float32)
    high = table.astype(jnp.bfloat16)
    low = (table - high.astype(np.float32)).astype(jnp.bfloat16)
    return jnp.asarray(high), jnp.asarray(low)


def split(x):
    high = x.astype(jnp.bfloat16)
    low = (x - high.astype(jnp.float32)).astype(jnp.bfloat16)
    return high, low


def dot(a, b, dims):
    return lax.dot_general(a, b, dims, preferred_element_type=jnp.float32)


def left_lanes(shape):
    return lax.broadcasted_iota(jnp.int32, shape, len(shape) - 1) < LANES // 2


def swap(x):
    return pltpu.roll(x, LANES // 2, len(x.shape) - 1)


def pack_kernel(base, state_ref, near_ref, far_ref, sums_ref):
    rows = state_ref.shape[2]
    even = jnp.bitwise_and(lax.axis_index("gx"), 1) == 0
    left = left_lanes((rows, LANES))
    totals = []
    for e in range(GROUP):
        acc = jnp.zeros((rows, LANES), jnp.float32)
        for p in range(2):
            a = state_ref[base + e, p]
            b = state_ref[base + e, p + 2]
            acc += a * a + b * b
            last = jnp.where(left, swap(a), b)
            first = jnp.where(left, a, swap(b))
            near_ref[e, p] = jnp.where(even, last, first)
            far_ref[e, p] = jnp.where(even, first, last)
        totals.append(jnp.sum(acc))
    half = left_lanes((4, LANES))
    for q in range(GROUP // 2):
        sums_ref[4 * q : 4 * q + 4] = jnp.where(half, totals[2 * q], totals[2 * q + 1])


def peers(parts):
    me = lax.axis_index("gy")
    return [jnp.bitwise_xor(me, d) for d in range(parts)]


def reorder_lanes(x):
    me = lax.axis_index("gy")
    far = jnp.bitwise_and(me, 2) != 0
    near = jnp.bitwise_and(me, 1) != 0
    a, b = x[..., :LANES], x[..., LANES:]
    a, b = jnp.where(far, b, a), jnp.where(far, a, b)
    return jnp.where(near, swap(a), a), jnp.where(near, swap(b), b)


def split_kernel(inverse_ref, high_ref, low_ref):
    coef_count = inverse_ref.shape[1]
    coef = LANES // 2
    for d, peer in enumerate(peers(coef_count // coef)):
        rows = pl.ds(pl.multiple_of(peer * coef, coef), coef)
        for h, x in enumerate(reorder_lanes(inverse_ref[:, rows, :])):
            at = (slice(None), slice(d * coef, (d + 1) * coef), slice(h * LANES, (h + 1) * LANES))
            high_ref[at], low_ref[at] = split(x)


def project_kernel(base, state_ref, near_ref, far_ref, high_ref, low_ref, *out_refs):
    parts = len(out_refs)
    slots, rows, _ = out_refs[0].shape
    coef = state_ref.shape[2]
    count = slots * parts
    lane = lax.broadcasted_iota(jnp.int32, (1, GROUP * coef), 1)
    index = lax.axis_index("gy") * coef + lax.rem(lane, coef)
    interior = index < coef * parts - 2
    even = jnp.bitwise_and(lax.axis_index("gx"), 1) == 0
    where = [pl.multiple_of(peer * slots, slots) for peer in peers(parts)]
    for p in range(2):
        near = near_ref[:, p].reshape(GROUP * coef, LANES)
        far = far_ref[:, p].reshape(GROUP * coef, LANES)
        x = jnp.concatenate(
            [
                state_ref[base : base + GROUP, p].reshape(GROUP * coef, LANES),
                state_ref[base : base + GROUP, p + 2].reshape(GROUP * coef, LANES),
                jnp.where(even, far, near),
                jnp.where(even, near, far),
            ],
            axis=1,
        )
        x_high, x_low = split(x)
        w_high, w_low = [
            jnp.concatenate(
                [ref[p, pl.ds(f * count + at, slots), :] for f in range(2) for at in where], axis=0
            )
            for ref in (high_ref, low_ref)
        ]
        t = dot(w_high, x_high, NT) + (dot(w_high, x_low, NT) + dot(w_low, x_high, NT))
        t = jnp.where(interior, t, 0.0)
        for d in range(parts):
            flat = out_refs[d].reshape(slots * rows, LANES)
            for f in range(2):
                first = f * count + d * slots
                for q in range(GROUP // 2):
                    flat[pl.ds(4 * q + p + 2 * f, slots, stride=rows), :] = t[
                        first : first + slots, q * LANES : (q + 1) * LANES
                    ]


def solve_kernel(parts, *refs):
    recv_refs = refs[:parts]
    high_ref, low_ref, wall_ref = refs[parts : parts + 3]
    out_refs = refs[parts + 3 :]
    slots, rows, _ = recv_refs[0].shape
    left = left_lanes((rows, LANES))
    lane = lax.broadcasted_iota(jnp.int32, (rows, LANES), 1)
    wall = jnp.concatenate(reorder_lanes(wall_ref[...]), axis=1)
    sums = jnp.zeros((rows, LANES), jnp.float32)
    for m in range(slots):
        t = [ref[m] for ref in recv_refs]
        even, odd = [], []
        for d in range(0, parts, 2):
            even.append(jnp.where(left, t[d], swap(t[d + 1])))
            odd.append(jnp.where(left, swap(t[d]), t[d + 1]))
        r = jnp.concatenate(
            [jnp.concatenate(even, axis=1), jnp.concatenate(odd, axis=1)], axis=0
        )
        r_high, r_low = split(r)
        v_high = high_ref[m]
        v_low = low_ref[m]
        both = dot(jnp.concatenate([r_high, r_low], axis=0), v_high, NT)
        o = both[: 2 * rows] + (both[2 * rows :] + dot(r_high, v_low, NT))
        for d in range(0, parts, 2):
            a = o[:rows, d * 64 : d * 64 + LANES]
            b = o[rows:, d * 64 : d * 64 + LANES]
            out_refs[d][m] = jnp.where(left, a, swap(b))
            out_refs[d + 1][m] = jnp.where(left, swap(a), b)
        for w in range(2):
            q = jnp.sum(o * wall[w : w + 1], axis=1, keepdims=True)
            for e in range(2):
                at = e * 2 * slots + w * slots + m
                sums = jnp.where(lane == at, q[e * rows : (e + 1) * rows], sums)
    for ref in out_refs:
        ref[slots] = sums


def back_kernel(total, base, parts, *refs):
    recv_refs = refs[:parts]
    high_ref, low_ref, sums_ref = refs[parts : parts + 3]
    out_ref, wall_ref = refs[-2:]
    slots, rows, _ = recv_refs[0].shape
    coef = out_ref.shape[2]
    width = slots - 1
    where = [pl.multiple_of(peer * width, width) for peer in peers(parts)]
    b_high, b_low = [
        jnp.concatenate([ref[pl.ds(at, width), :] for at in where], axis=0)
        for ref in (high_ref, low_ref)
    ]
    me = lax.axis_index("gy")
    near = jnp.bitwise_and(me, 1) != 0
    far = jnp.bitwise_and(me, 2) != 0
    scale = lax.rsqrt(sums_ref[base : base + rows] / total + EPSILON)
    for r in range(rows):
        q, f = r // 4, r % 4
        s = jnp.concatenate(
            [
                ref.reshape(slots * rows, LANES)[pl.ds(r, width, stride=rows), :]
                for ref in recv_refs
            ],
            axis=0,
        )
        s = (s * scale[r : r + 1]).T
        s_high, s_low = split(s)
        o = dot(s_high, b_high, NN) + (dot(s_high, b_low, NN) + dot(s_low, b_high, NN))
        for e in range(2):
            out_ref[2 * q + e, f] = o[e * coef : (e + 1) * coef]
    lane = lax.broadcasted_iota(jnp.int32, (rows, LANES), 1)
    tiles = [ref[slots - 1] for ref in recv_refs]
    tiles = [jnp.where(near, tiles[d ^ 1], tiles[d]) for d in range(parts)]
    tiles = [jnp.where(far, tiles[d ^ 2], tiles[d]) * scale for d in range(parts)]
    b_high = high_ref[...]
    b_low = low_ref[...]
    for e in range(2):
        for w in range(2):
            g = jnp.zeros((rows, LANES), jnp.float32)
            for k in range(parts):
                shift = (k * width - (e * 2 + w) * width) % LANES
                tile = pltpu.roll(tiles[k], shift, 1) if shift else tiles[k]
                g = jnp.where((lane >= k * width) & (lane < (k + 1) * width), tile, g)
            g_high, g_low = split(g)
            o = dot(g_high, b_high, NN) + (dot(g_high, b_low, NN) + dot(g_low, b_high, NN))
            for q in range(GROUP // 2):
                for c in range(2):
                    row = 4 * q + 2 * c
                    wall_ref[2 * q + e, w, c : c + 1] = o[row : row + 1]


def exchanged(pieces, axis):
    n = lax.axis_size(axis)
    got = list(pieces)
    for d in range(n - 1, 0, -1):
        got[d] = lax.ppermute(pieces[d], axis, [(i, i ^ d) for i in range(n)])
    return got


def halo_pairs(n):
    near = [(i, i ^ 1) for i in range(n)]
    far = [(i, (i + (1 if i % 2 else -1)) % n) for i in range(n)]
    return near, far


def axis_hops(n):
    return [1 << i for i in range(n.bit_length() - 1)]


def full_sum(x):
    for axis in ("gx", "gy"):
        n = lax.axis_size(axis)
        for hop in axis_hops(n):
            other = lax.ppermute(x, axis, [(i, i ^ hop) for i in range(n)])
            x = x + other
    return x


def per_device(state, inverse):
    members, fields, coef, points = state.shape
    parts = lax.axis_size("gy")
    coef_count = coef * parts
    grid_x = points * lax.axis_size("gx")
    window = points + 2 * HALO
    mine = MODES // parts
    group_rows = GROUP * fields * coef // LANES
    groups = members // GROUP

    values, slopes, back_table = window_tables(window, HALO, points, MODES)
    step_high, step_low = split_table(step_tables(values, slopes, HALO, points))
    back_high, back_low = split_table(back_table)
    k = np.arange(coef_count)
    curvature = k * k / (coef_count * coef_count)
    wall = np.zeros((8, coef_count), np.float32)
    wall[0] = curvature
    wall[1] = np.where(k % 2 == 0, -1.0, 1.0) * curvature
    wall = jnp.asarray(wall)

    def grouped(g, shape):
        return pl.BlockSpec((GROUP,) + shape, lambda i: (g,) + (0,) * len(shape))

    def call(kernel, vmem, flops, moved, **kwargs):
        return pl.pallas_call(
            kernel,
            compiler_params=pltpu.CompilerParams(vmem_limit_bytes=vmem * MIB),
            cost_estimate=pl.CostEstimate(flops=flops, bytes_accessed=moved, transcendentals=0),
            **kwargs,
        )

    block = (fields, coef, points)
    halo = (GROUP, 2, coef, LANES)
    halo_bytes = 4 * int(np.prod(halo))
    small = (group_rows, LANES)
    sent_shape = (mine, group_rows, LANES)
    back_shape = (mine + 1, group_rows, LANES)

    packed = []
    for g in range(groups):
        packed.append(
            call(
                functools.partial(pack_kernel, g * GROUP),
                6,
                10**6,
                4 * halo_bytes,
                in_specs=[VMEM],
                out_specs=[VMEM] * 3,
                out_shape=[
                    jax.ShapeDtypeStruct(halo, jnp.float32),
                    jax.ShapeDtypeStruct(halo, jnp.float32),
                    jax.ShapeDtypeStruct(small, jnp.float32),
                ],
            )(state)
        )
    halos = []
    near_pairs, far_pairs = halo_pairs(lax.axis_size("gx"))
    for near, far, _ in packed:
        near = lax.ppermute(near, "gx", near_pairs)
        far = lax.ppermute(far, "gx", far_pairs)
        halos.append((near, far))
    sums = full_sum(jnp.concatenate([p[2] for p in packed], axis=0))

    per_step = 4
    split_shape = (per_step, coef_count, coef_count)
    inverse_high, inverse_low = pl.pallas_call(
        split_kernel,
        grid=(mine // per_step,),
        in_specs=[pl.BlockSpec(split_shape, lambda i: (i, 0, 0))],
        out_specs=[pl.BlockSpec(split_shape, lambda i: (i, 0, 0))] * 2,
        out_shape=[jax.ShapeDtypeStruct(inverse.shape, jnp.bfloat16)] * 2,
        name="split",
        compiler_params=pltpu.CompilerParams(vmem_limit_bytes=8 * MIB),
        cost_estimate=pl.CostEstimate(
            flops=10**7, bytes_accessed=8 * mine * coef_count**2, transcendentals=0
        ),
    )(inverse)

    outputs = []
    for g in range(groups):
        sent = call(
            functools.partial(project_kernel, g * GROUP),
            8,
            2 * 3 * 2 * 256 * 512 * GROUP * coef,
            6 * halo_bytes,
            in_specs=[VMEM] * 5,
            out_specs=[VMEM] * parts,
            out_shape=[jax.ShapeDtypeStruct(sent_shape, jnp.float32)] * parts,
        )(state, *halos[g], step_high, step_low)
        got = exchanged(sent, "gy")
        solved = call(
            functools.partial(solve_kernel, parts),
            6,
            2 * 3 * mine * coef_count**2 * 256,
            4 * mine * coef_count**2,
            in_specs=[VMEM] * (parts + 3),
            out_specs=[VMEM] * parts,
            out_shape=[jax.ShapeDtypeStruct(back_shape, jnp.float32)] * parts,
        )(*got, inverse_high, inverse_low, wall)
        returned = exchanged(solved, "gy")
        outputs = call(
            functools.partial(back_kernel, float(fields * coef_count * grid_x), g * group_rows, parts),
            8,
            2 * 3 * 128 * 128 * GROUP * fields * coef,
            4 * halo_bytes,
            grid=(1,),
            in_specs=[VMEM] * (parts + 3)
            + [pl.BlockSpec(memory_space=pl.ANY)] * len(outputs),
            out_specs=[grouped(g, block), grouped(g, (2, 2, points))],
            out_shape=[
                jax.ShapeDtypeStruct(state.shape, jnp.float32),
                jax.ShapeDtypeStruct((members, 2, 2, points), jnp.float32),
            ],
            input_output_aliases={parts + 3 + i: i for i in range(len(outputs))},
        )(*returned, back_high, back_low, sums, *outputs)
    return tuple(outputs)


def solution(mesh):
    placed = (P(None, None, "gy", "gx"), P("gy", None, None))

    return jax.shard_map(
        per_device,
        mesh=mesh,
        in_specs=placed,
        out_specs=(P(None, None, "gy", "gx"), P(None, None, None, "gx")),
        check_vma=False,
    )
```

```python
import functools
import math

import jax
import jax.numpy as jnp
import numpy as np
from jax import lax
from jax.experimental import pallas as pl
from jax.experimental.pallas import tpu as pltpu
from jax.sharding import PartitionSpec as P


MODES = 128
HALO = 64

EPSILON = 1e-06
TIME_STEP = 0.5
MEAN_FLOW = 0.8
CORIOLIS = 0.6
STRATIFICATION = 0.9

LANES = 128
MIB = 1 << 20
TILE = 8
VMEM = pl.BlockSpec(memory_space=pltpu.VMEM)
ANY = pl.BlockSpec(memory_space=pl.ANY)
NT = (((1,), (1,)), ((), ()))
NN = (((1,), (0,)), ((), ()))


def window_tables(window, rim_width, points, mode_count):
    position = np.arange(window)
    mode_index = np.arange(mode_count)
    half_count = mode_count // 2
    is_cosine = mode_index <= half_count
    wave_index = np.where(is_cosine, mode_index, mode_index - half_count)
    product_index = position[:, None] * wave_index[None, :] % window
    phases = 2.0 * np.pi * product_index / window
    weights_norm = np.where(wave_index == 0, np.sqrt(1.0 / window), np.sqrt(2.0 / window))
    basis = np.where(is_cosine[None, :], np.cos(phases), np.sin(phases)) * weights_norm[None, :]
    wavenumber = 2.0 * np.pi * wave_index / window
    paired = wave_index[:, None] == wave_index[None, :]
    to_sine = is_cosine[:, None] & ~is_cosine[None, :] & paired
    to_cosine = ~is_cosine[:, None] & is_cosine[None, :] & paired
    derivative = np.where(to_sine, -wavenumber[:, None], 0.0) + np.where(
        to_cosine, wavenumber[:, None], 0.0
    )
    taper = 0.25 + 0.75 * np.sin(np.pi * (position + 0.5) / window) ** 2
    values = basis * taper[:, None]
    slopes = (basis @ derivative) * taper[:, None]
    back_table = (
        basis[rim_width : rim_width + points, :] / taper[rim_width : rim_width + points, None]
    ).T
    return values, slopes, back_table


def step_tables(values, slopes, rim, points):
    direct = values - TIME_STEP * MEAN_FLOW * slopes
    couplings = (
        (TIME_STEP * CORIOLIS, -TIME_STEP * CORIOLIS),
        (TIME_STEP, -TIME_STEP * STRATIFICATION),
    )
    tables = []
    for to_first, to_second in couplings:
        first = (direct, to_first * values)
        second = (to_second * values, direct)
        rows = []
        for part in (first, second):
            pieces = []
            for begin, end in ((rim, rim + points), (0, rim), (rim + points, points + 2 * rim)):
                pieces += [part[0][begin:end].T, part[1][begin:end].T]
            rows.append(np.concatenate(pieces, axis=1))
        tables.append(np.concatenate(rows, axis=0))
    return np.stack(tables)


def split_table(table):
    table = np.asarray(table, np.float32)
    high = table.astype(jnp.bfloat16)
    low = (table - high.astype(np.float32)).astype(jnp.bfloat16)
    return jnp.asarray(high), jnp.asarray(low)


def split(x):
    high = x.astype(jnp.bfloat16)
    low = (x - high.astype(jnp.float32)).astype(jnp.bfloat16)
    return high, low


def dot(a, b, dims):
    return lax.dot_general(a, b, dims, preferred_element_type=jnp.float32)


def left_lanes(shape):
    return lax.broadcasted_iota(jnp.int32, shape, len(shape) - 1) < LANES // 2


def swap(x):
    return pltpu.roll(x, LANES // 2, len(x.shape) - 1)


def pack_kernel(base, state_ref, near_ref, far_ref):
    rows = state_ref.shape[2]
    even = jnp.bitwise_and(lax.axis_index("gx"), 1) == 0
    left = left_lanes((rows, LANES))
    for e in range(near_ref.shape[0]):
        for p in range(2):
            a = state_ref[base + e, p]
            b = state_ref[base + e, p + 2]
            last = jnp.where(left, swap(a), b)
            first = jnp.where(left, a, swap(b))
            near_ref[e, p] = jnp.where(even, last, first)
            far_ref[e, p] = jnp.where(even, first, last)


def squares_kernel(state_ref, sums_ref):
    members, fields, rows, _ = state_ref.shape
    half = left_lanes((fields, LANES))
    for q in range(members // 2):
        totals = []
        for e in range(2):
            acc = jnp.zeros((rows, LANES), jnp.float32)
            for f in range(fields):
                a = state_ref[2 * q + e, f]
                acc += a * a
            totals.append(jnp.sum(acc))
        sums_ref[fields * q : fields * (q + 1)] = jnp.where(half, totals[0], totals[1])


def peers(parts):
    me = lax.axis_index("gy")
    return [jnp.bitwise_xor(me, d) for d in range(parts)]


def reorder_lanes(x):
    me = lax.axis_index("gy")
    far = jnp.bitwise_and(me, 2) != 0
    near = jnp.bitwise_and(me, 1) != 0
    a, b = x[..., :LANES], x[..., LANES:]
    a, b = jnp.where(far, b, a), jnp.where(far, a, b)
    return jnp.where(near, swap(a), a), jnp.where(near, swap(b), b)


def split_kernel(inverse_ref, high_ref, low_ref):
    coef_count = inverse_ref.shape[1]
    coef = LANES // 2
    for d, peer in enumerate(peers(coef_count // coef)):
        rows = pl.ds(pl.multiple_of(peer * coef, coef), coef)
        for h, x in enumerate(reorder_lanes(inverse_ref[:, rows, :])):
            at = (slice(None), slice(d * coef, (d + 1) * coef), slice(h * LANES, (h + 1) * LANES))
            high_ref[at], low_ref[at] = split(x)


def project_kernel(base, state_ref, near_ref, far_ref, high_ref, low_ref, *out_refs):
    parts = len(out_refs)
    members, _, coef, _ = near_ref.shape
    rows = 2 * members
    slots = out_refs[0].shape[0] // rows
    count = slots * parts
    lane = lax.broadcasted_iota(jnp.int32, (1, members * coef), 1)
    index = lax.axis_index("gy") * coef + lax.rem(lane, coef)
    interior = index < coef * parts - 2
    even = jnp.bitwise_and(lax.axis_index("gx"), 1) == 0
    where = [pl.multiple_of(peer * slots, slots) for peer in peers(parts)]
    for p in range(2):
        near = near_ref[:, p].reshape(members * coef, LANES)
        far = far_ref[:, p].reshape(members * coef, LANES)
        x = jnp.concatenate(
            [
                state_ref[base : base + members, p].reshape(members * coef, LANES),
                state_ref[base : base + members, p + 2].reshape(members * coef, LANES),
                jnp.where(even, far, near),
                jnp.where(even, near, far),
            ],
            axis=1,
        )
        x_high, x_low = split(x)
        w_high, w_low = [
            jnp.concatenate(
                [ref[p, pl.ds(f * count + at, slots), :] for f in range(2) for at in where], axis=0
            )
            for ref in (high_ref, low_ref)
        ]
        t = dot(w_high, x_high, NT) + (dot(w_high, x_low, NT) + dot(w_low, x_high, NT))
        t = jnp.where(interior, t, 0.0)
        for d in range(parts):
            for f in range(2):
                first = f * count + d * slots
                for q in range(members // 2):
                    out_refs[d][pl.ds(4 * q + p + 2 * f, slots, stride=rows), :] = t[
                        first : first + slots, q * LANES : (q + 1) * LANES
                    ]


def solve_kernel(parts, rows, *refs):
    recv_refs = refs[:parts]
    high_refs, low_refs = refs[parts : parts + 2], refs[parts + 2 : parts + 4]
    wall_ref = refs[parts + 4]
    out_refs = refs[parts + 5 :]
    slots = recv_refs[0].shape[0] // rows
    modes = TILE // math.gcd(rows, TILE)
    unit = rows * modes
    left = left_lanes((unit, LANES))
    lane = lax.broadcasted_iota(jnp.int32, (unit, LANES), 1)
    mode = lax.broadcasted_iota(jnp.int32, (unit, LANES), 0) // rows
    wall = jnp.concatenate(reorder_lanes(wall_ref[...]), axis=1)
    sums = jnp.zeros((unit, LANES), jnp.float32)
    for i in range(slots // modes):
        tile = slice(i * unit, (i + 1) * unit)
        t = [ref[tile] for ref in recv_refs]
        even, odd = [], []
        for d in range(0, parts, 2):
            even.append(jnp.where(left, t[d], swap(t[d + 1])))
            odd.append(jnp.where(left, swap(t[d]), t[d + 1]))
        even = jnp.concatenate(even, axis=1)
        odd = jnp.concatenate(odd, axis=1)
        solved = []
        for j in range(modes):
            r = jnp.concatenate([x[j * rows : (j + 1) * rows] for x in (even, odd)], axis=0)
            half, at = divmod(i * modes + j, high_refs[0].shape[0])
            v_high = high_refs[half][at]
            v_low = low_refs[half][at]
            r_high, r_low = split(r)
            both = dot(jnp.concatenate([r_high, r_low], axis=0), v_high, NT)
            solved.append(both[: 2 * rows] + (both[2 * rows :] + dot(r_high, v_low, NT)))
        even = jnp.concatenate([o[:rows] for o in solved], axis=0)
        odd = jnp.concatenate([o[rows:] for o in solved], axis=0)
        for d in range(0, parts, 2):
            a = even[:, d * LANES // 2 : d * LANES // 2 + LANES]
            b = odd[:, d * LANES // 2 : d * LANES // 2 + LANES]
            out_refs[d][tile] = jnp.where(left, a, swap(b))
            out_refs[d + 1][tile] = jnp.where(left, swap(a), b)
        for e, o in enumerate((even, odd)):
            for w in range(2):
                q = jnp.sum(o * wall[w : w + 1], axis=1, keepdims=True)
                sums = jnp.where(lane == (2 * e + w) * slots + i * modes + mode, q, sums)
    total = sums[:rows]
    for j in range(1, modes):
        total = total + sums[j * rows : (j + 1) * rows]
    for ref in out_refs:
        ref[slots * rows : slots * rows + rows] = total
        if rows % TILE:
            spare = ref.shape[0] - (slots + 1) * rows
            ref[(slots + 1) * rows :] = jnp.zeros((spare, LANES), jnp.float32)


def back_kernel(count, first, slots, parts, *refs):
    recv_refs = refs[:parts]
    high_ref, low_ref, sums_ref = refs[parts : parts + 3]
    out_ref, wall_ref, values_ref, stress_ref, sems = refs[-5:]
    members, fields, coef, _ = values_ref.shape
    rows = 2 * members
    base = 2 * first
    where = [pl.multiple_of(peer * slots, slots) for peer in peers(parts)]
    b_high, b_low = [
        jnp.concatenate([ref[pl.ds(at, slots), :] for at in where], axis=0)
        for ref in (high_ref, low_ref)
    ]
    scale = lax.rsqrt(sums_ref[base : base + rows] / count + EPSILON)
    copies = []
    for r in range(rows):
        q, f = divmod(r, fields)
        s = jnp.concatenate([ref[pl.ds(r, slots, stride=rows), :] for ref in recv_refs], axis=0)
        s = (s * scale[r : r + 1]).T
        s_high, s_low = split(s)
        o = dot(s_high, b_high, NN) + (dot(s_high, b_low, NN) + dot(s_low, b_high, NN))
        for e in range(2):
            values_ref[2 * q + e, f] = o[e * coef : (e + 1) * coef]
        if f == fields - 1:
            pair = pl.ds(2 * q, 2)
            copies.append(
                pltpu.make_async_copy(
                    values_ref.at[pair], out_ref.at[pl.ds(first + 2 * q, 2)], sems.at[q]
                )
            )
            copies[-1].start()
    me = lax.axis_index("gy")
    near = jnp.bitwise_and(me, 1) != 0
    far = jnp.bitwise_and(me, 2) != 0
    lane = lax.broadcasted_iota(jnp.int32, (rows, LANES), 1)
    tiles = [ref[slots * rows : slots * rows + rows] for ref in recv_refs]
    tiles = [jnp.where(near, tiles[d ^ 1], tiles[d]) for d in range(parts)]
    tiles = [jnp.where(far, tiles[d ^ 2], tiles[d]) * scale for d in range(parts)]
    b_high = high_ref[...]
    b_low = low_ref[...]
    for e in range(2):
        for w in range(2):
            g = jnp.zeros((rows, LANES), jnp.float32)
            for k in range(parts):
                shift = (k * slots - (e * 2 + w) * slots) % LANES
                tile = pltpu.roll(tiles[k], shift, 1) if shift else tiles[k]
                g = jnp.where((lane >= k * slots) & (lane < (k + 1) * slots), tile, g)
            g_high, g_low = split(g)
            o = dot(g_high, b_high, NN) + (dot(g_high, b_low, NN) + dot(g_low, b_high, NN))
            for q in range(members // 2):
                for c in range(2):
                    row = fields * q + 2 * c
                    stress_ref[2 * q + e, w, c : c + 1] = o[row : row + 1]
    copies.append(
        pltpu.make_async_copy(
            stress_ref, wall_ref.at[pl.ds(first, members)], sems.at[members // 2]
        )
    )
    copies[-1].start()
    for copy in copies:
        copy.wait()


def exchanged(pieces, axis):
    n = lax.axis_size(axis)
    got = list(pieces)
    for d in range(n - 1, 0, -1):
        got[d] = lax.ppermute(pieces[d], axis, [(i, i ^ d) for i in range(n)])
    return got


def halo_pairs(n):
    near = [(i, i ^ 1) for i in range(n)]
    far = [(i, (i + (1 if i % 2 else -1)) % n) for i in range(n)]
    return near, far


def axis_hops(n):
    return [1 << i for i in range(n.bit_length() - 1)]


def full_sum(x):
    for axis in ("gy", "gx"):
        n = lax.axis_size(axis)
        for hop in axis_hops(n):
            other = lax.ppermute(x, axis, [(i, i ^ hop) for i in range(n)])
            x = x + other
    return x


SIZES = (4, 4, 4)


def chunks(members):
    sizes = SIZES if sum(SIZES) == members else (2,) * (members // 2)
    return [(sum(sizes[:g]), count) for g, count in enumerate(sizes)]


def per_device(state, inverse):
    members, fields, coef, points = state.shape
    parts = lax.axis_size("gy")
    coef_count = coef * parts
    grid_x = points * lax.axis_size("gx")
    window = points + 2 * HALO
    mine = MODES // parts
    plan = chunks(members)

    values, slopes, back_table = window_tables(window, HALO, points, MODES)
    step_high, step_low = split_table(step_tables(values, slopes, HALO, points))
    back_high, back_low = split_table(back_table)
    k = np.arange(coef_count)
    curvature = k * k / (coef_count * coef_count)
    wall = np.zeros((TILE, coef_count), np.float32)
    wall[0] = curvature
    wall[1] = np.where(k % 2 == 0, -1.0, 1.0) * curvature
    wall = jnp.asarray(wall)

    def call(kernel, vmem, flops, moved, **kwargs):
        return pl.pallas_call(
            kernel,
            compiler_params=pltpu.CompilerParams(vmem_limit_bytes=vmem * MIB),
            cost_estimate=pl.CostEstimate(flops=flops, bytes_accessed=moved, transcendentals=0),
            **kwargs,
        )

    def array(*shape):
        return jax.ShapeDtypeStruct(shape, jnp.float32)

    member_bytes = 4 * fields * coef * points
    packed = []
    for first, count in plan:
        packed.append(
            call(
                functools.partial(pack_kernel, first),
                6,
                10**6,
                2 * count * member_bytes,
                in_specs=[VMEM],
                out_specs=[VMEM] * 2,
                out_shape=[array(count, 2, coef, LANES)] * 2,
            )(state)
        )
    squares = call(
        squares_kernel,
        6,
        10**9,
        10**7,
        in_specs=[VMEM],
        out_specs=VMEM,
        out_shape=array(2 * members, LANES),
    )(state)
    halos = []
    near_pairs, far_pairs = halo_pairs(lax.axis_size("gx"))
    for near, far in packed:
        near = lax.ppermute(near, "gx", near_pairs)
        far = lax.ppermute(far, "gx", far_pairs)
        halos.append((near, far))
    sums = full_sum(squares)

    per_step = 4
    steps = mine // per_step // 2
    split_shape = (per_step, coef_count, coef_count)
    high, low = [], []
    for h in range(2):
        out = call(
            split_kernel,
            8,
            10**7,
            4 * mine * coef_count**2,
            grid=(steps,),
            in_specs=[pl.BlockSpec(split_shape, lambda i, h=h: (h * steps + i, 0, 0))],
            out_specs=[pl.BlockSpec(split_shape, lambda i: (i, 0, 0))] * 2,
            out_shape=[jax.ShapeDtypeStruct((mine // 2,) + split_shape[1:], jnp.bfloat16)] * 2,
        )(inverse)
        high.append(out[0])
        low.append(out[1])

    outputs = []
    for g, (first, count) in enumerate(plan):
        rows = count * fields // 2
        sent = call(
            functools.partial(project_kernel, first),
            8,
            3 * 2 * 2 * (2 * MODES) * (4 * LANES) * count * coef,
            3 * count * member_bytes,
            in_specs=[VMEM] * 5,
            out_specs=[VMEM] * parts,
            out_shape=[array(mine * rows, LANES)] * parts,
        )(state, *halos[g], step_high, step_low)
        got = exchanged(sent, "gy")
        solved = call(
            functools.partial(solve_kernel, parts, rows),
            6,
            3 * 2 * mine * coef_count**2 * 256,
            4 * mine * coef_count**2,
            in_specs=[VMEM] * (parts + 5),
            out_specs=[VMEM] * parts,
            out_shape=[array((mine + 1) * rows + -(mine + 1) * rows % TILE, LANES)] * parts,
        )(*got, *high, *low, wall)
        returned = exchanged(solved, "gy")

        outputs = call(
            functools.partial(
                back_kernel, float(fields * coef_count * grid_x), first, mine, parts
            ),
            8,
            3 * 2 * MODES * points * count * fields * coef,
            2 * count * member_bytes,
            in_specs=[VMEM] * (parts + 3) + [ANY] * len(outputs),
            out_specs=[ANY] * 2,
            out_shape=[array(*state.shape), array(members, 2, 2, points)],
            scratch_shapes=[
                pltpu.VMEM((count, fields, coef, points), jnp.float32),
                pltpu.VMEM((count, 2, 2, points), jnp.float32),
                pltpu.SemaphoreType.DMA((count // 2 + 1,)),
            ],
            input_output_aliases={parts + 3 + i: i for i in range(len(outputs))},
        )(*returned, back_high, back_low, sums, *outputs)
    return tuple(outputs)


def solution(mesh):
    placed = (P(None, None, "gy", "gx"), P("gy", None, None))

    return jax.shard_map(
        per_device,
        mesh=mesh,
        in_specs=placed,
        out_specs=(P(None, None, "gy", "gx"), P(None, None, None, "gx")),
        check_vma=False,
    )
```

```python
import functools
import math

import jax
import jax.numpy as jnp
import numpy as np
from jax import lax
from jax.experimental import pallas as pl
from jax.experimental.pallas import tpu as pltpu
from jax.sharding import PartitionSpec as P


MODES = 128
HALO = 64

EPSILON = 1e-06
TIME_STEP = 0.5
MEAN_FLOW = 0.8
CORIOLIS = 0.6
STRATIFICATION = 0.9

LANES = 128
MIB = 1 << 20
TILE = 8
VMEM = pl.BlockSpec(memory_space=pltpu.VMEM)
ANY = pl.BlockSpec(memory_space=pl.ANY)
NT = (((1,), (1,)), ((), ()))
NN = (((1,), (0,)), ((), ()))


def window_tables(window, rim_width, points, mode_count):
    position = np.arange(window)
    mode_index = np.arange(mode_count)
    half_count = mode_count // 2
    is_cosine = mode_index <= half_count
    wave_index = np.where(is_cosine, mode_index, mode_index - half_count)
    product_index = position[:, None] * wave_index[None, :] % window
    phases = 2.0 * np.pi * product_index / window
    weights_norm = np.where(wave_index == 0, np.sqrt(1.0 / window), np.sqrt(2.0 / window))
    basis = np.where(is_cosine[None, :], np.cos(phases), np.sin(phases)) * weights_norm[None, :]
    wavenumber = 2.0 * np.pi * wave_index / window
    paired = wave_index[:, None] == wave_index[None, :]
    to_sine = is_cosine[:, None] & ~is_cosine[None, :] & paired
    to_cosine = ~is_cosine[:, None] & is_cosine[None, :] & paired
    derivative = np.where(to_sine, -wavenumber[:, None], 0.0) + np.where(
        to_cosine, wavenumber[:, None], 0.0
    )
    taper = 0.25 + 0.75 * np.sin(np.pi * (position + 0.5) / window) ** 2
    values = basis * taper[:, None]
    slopes = (basis @ derivative) * taper[:, None]
    back_table = (
        basis[rim_width : rim_width + points, :] / taper[rim_width : rim_width + points, None]
    ).T
    return values, slopes, back_table


def step_tables(values, slopes, rim, points):
    direct = values - TIME_STEP * MEAN_FLOW * slopes
    couplings = (
        (TIME_STEP * CORIOLIS, -TIME_STEP * CORIOLIS),
        (TIME_STEP, -TIME_STEP * STRATIFICATION),
    )
    tables = []
    for to_first, to_second in couplings:
        first = (direct, to_first * values)
        second = (to_second * values, direct)
        rows = []
        for part in (first, second):
            pieces = []
            for begin, end in ((rim, rim + points), (0, rim), (rim + points, points + 2 * rim)):
                pieces += [part[0][begin:end].T, part[1][begin:end].T]
            rows.append(np.concatenate(pieces, axis=1))
        tables.append(np.concatenate(rows, axis=0))
    return np.stack(tables)


def split_table(table):
    table = np.asarray(table, np.float32)
    high = table.astype(jnp.bfloat16)
    low = (table - high.astype(np.float32)).astype(jnp.bfloat16)
    return jnp.asarray(high), jnp.asarray(low)


def split(x):
    high = x.astype(jnp.bfloat16)
    low = (x - high.astype(jnp.float32)).astype(jnp.bfloat16)
    return high, low


def dot(a, b, dims):
    return lax.dot_general(a, b, dims, preferred_element_type=jnp.float32)


def left_lanes(shape):
    return lax.broadcasted_iota(jnp.int32, shape, len(shape) - 1) < LANES // 2


def swap(x):
    return pltpu.roll(x, LANES // 2, len(x.shape) - 1)


def pack_kernel(base, state_ref, near_ref, far_ref):
    rows = state_ref.shape[2]
    even = jnp.bitwise_and(lax.axis_index("gx"), 1) == 0
    left = left_lanes((rows, LANES))
    for e in range(near_ref.shape[0]):
        for p in range(2):
            a = state_ref[base + e, p]
            b = state_ref[base + e, p + 2]
            last = jnp.where(left, swap(a), b)
            first = jnp.where(left, a, swap(b))
            near_ref[e, p] = jnp.where(even, last, first)
            far_ref[e, p] = jnp.where(even, first, last)


def squares_kernel(state_ref, sums_ref):
    members, fields, rows, _ = state_ref.shape
    half = left_lanes((fields, LANES))
    for q in range(members // 2):
        totals = []
        for e in range(2):
            acc = jnp.zeros((rows, LANES), jnp.float32)
            for f in range(fields):
                a = state_ref[2 * q + e, f]
                acc += a * a
            totals.append(jnp.sum(acc))
        sums_ref[fields * q : fields * (q + 1)] = jnp.where(half, totals[0], totals[1])


def peers(parts):
    me = lax.axis_index("gy")
    return [jnp.bitwise_xor(me, d) for d in range(parts)]


def reorder_lanes(x):
    me = lax.axis_index("gy")
    far = jnp.bitwise_and(me, 2) != 0
    near = jnp.bitwise_and(me, 1) != 0
    a, b = x[..., :LANES], x[..., LANES:]
    a, b = jnp.where(far, b, a), jnp.where(far, a, b)
    return jnp.where(near, swap(a), a), jnp.where(near, swap(b), b)


def split_kernel(inverse_ref, high_ref, low_ref):
    coef_count = inverse_ref.shape[1]
    coef = LANES // 2
    for d, peer in enumerate(peers(coef_count // coef)):
        rows = pl.ds(pl.multiple_of(peer * coef, coef), coef)
        for h, x in enumerate(reorder_lanes(inverse_ref[:, rows, :])):
            at = (slice(None), slice(d * coef, (d + 1) * coef), slice(h * LANES, (h + 1) * LANES))
            high_ref[at], low_ref[at] = split(x)


def project_kernel(base, state_ref, near_ref, far_ref, high_ref, low_ref, *out_refs):
    parts = len(out_refs)
    members, _, coef, _ = near_ref.shape
    rows = 2 * members
    slots = out_refs[0].shape[0] // rows
    count = slots * parts
    lane = lax.broadcasted_iota(jnp.int32, (1, members * coef), 1)
    index = lax.axis_index("gy") * coef + lax.rem(lane, coef)
    interior = index < coef * parts - 2
    even = jnp.bitwise_and(lax.axis_index("gx"), 1) == 0
    where = [pl.multiple_of(peer * slots, slots) for peer in peers(parts)]
    for p in range(2):
        near = near_ref[:, p].reshape(members * coef, LANES)
        far = far_ref[:, p].reshape(members * coef, LANES)
        x = jnp.concatenate(
            [
                state_ref[base : base + members, p].reshape(members * coef, LANES),
                state_ref[base : base + members, p + 2].reshape(members * coef, LANES),
                jnp.where(even, far, near),
                jnp.where(even, near, far),
            ],
            axis=1,
        )
        x_high, x_low = split(x)
        w_high, w_low = [
            jnp.concatenate(
                [ref[p, pl.ds(f * count + at, slots), :] for f in range(2) for at in where], axis=0
            )
            for ref in (high_ref, low_ref)
        ]
        t = dot(w_high, x_high, NT) + (dot(w_high, x_low, NT) + dot(w_low, x_high, NT))
        t = jnp.where(interior, t, 0.0)
        for d in range(parts):
            for f in range(2):
                first = f * count + d * slots
                for q in range(members // 2):
                    out_refs[d][pl.ds(4 * q + p + 2 * f, slots, stride=rows), :] = t[
                        first : first + slots, q * LANES : (q + 1) * LANES
                    ]


def products(i, h, rows, modes, recv_refs, high_refs, low_refs):
    unit = rows * modes
    left = left_lanes((unit, LANES))
    a, b = [ref[i * unit : (i + 1) * unit] for ref in recv_refs]
    even = jnp.where(left, a, swap(b))
    odd = jnp.where(left, swap(a), b)
    columns = slice(h * LANES, (h + 1) * LANES)
    found = []
    for j in range(modes):
        r = jnp.concatenate([x[j * rows : (j + 1) * rows] for x in (even, odd)], axis=0)
        half, at = divmod(i * modes + j, high_refs[0].shape[0])
        v_high = high_refs[half][at, :, columns]
        v_low = low_refs[half][at, :, columns]
        r_high, r_low = split(r)
        both = dot(jnp.concatenate([r_high, r_low], axis=0), v_high, NT)
        found.append(both[: 2 * rows] + (both[2 * rows :] + dot(r_high, v_low, NT)))
    return found


def begin_kernel(rows, *refs):
    recv_refs, high_refs, low_refs, out_ref = refs[:2], refs[2:4], refs[4:6], refs[6]
    modes = TILE // math.gcd(rows, TILE)
    for i in range(recv_refs[0].shape[0] // (rows * modes)):
        for j, o in enumerate(products(i, 0, rows, modes, recv_refs, high_refs, low_refs)):
            m = i * modes + j
            out_ref[m * 2 * rows : (m + 1) * 2 * rows] = o


def solve_kernel(parts, rows, *refs):
    recv_refs, high_refs, low_refs = refs[:2], refs[2:4], refs[4:6]
    begun_ref, wall_ref = refs[6:8]
    out_refs = refs[8:]
    slots = recv_refs[0].shape[0] // rows
    modes = TILE // math.gcd(rows, TILE)
    unit = rows * modes
    left = left_lanes((unit, LANES))
    lane = lax.broadcasted_iota(jnp.int32, (unit, LANES), 1)
    mode = lax.broadcasted_iota(jnp.int32, (unit, LANES), 0) // rows
    wall = jnp.concatenate(reorder_lanes(wall_ref[...]), axis=1)
    sums = jnp.zeros((unit, LANES), jnp.float32)
    for i in range(slots // modes):
        tile = slice(i * unit, (i + 1) * unit)
        solved = []
        for j, o in enumerate(products(i, 1, rows, modes, recv_refs, high_refs, low_refs)):
            m = i * modes + j
            solved.append(o + begun_ref[m * 2 * rows : (m + 1) * 2 * rows])
        even = jnp.concatenate([o[:rows] for o in solved], axis=0)
        odd = jnp.concatenate([o[rows:] for o in solved], axis=0)
        for d in range(0, parts, 2):
            a = even[:, d * LANES // 2 : d * LANES // 2 + LANES]
            b = odd[:, d * LANES // 2 : d * LANES // 2 + LANES]
            out_refs[d][tile] = jnp.where(left, a, swap(b))
            out_refs[d + 1][tile] = jnp.where(left, swap(a), b)
        for e, o in enumerate((even, odd)):
            for w in range(2):
                q = jnp.sum(o * wall[w : w + 1], axis=1, keepdims=True)
                sums = jnp.where(lane == (2 * e + w) * slots + i * modes + mode, q, sums)
    total = sums[:rows]
    for j in range(1, modes):
        total = total + sums[j * rows : (j + 1) * rows]
    for ref in out_refs:
        ref[slots * rows : slots * rows + rows] = total
        if rows % TILE:
            spare = ref.shape[0] - (slots + 1) * rows
            ref[(slots + 1) * rows :] = jnp.zeros((spare, LANES), jnp.float32)


def back_kernel(count, first, slots, parts, *refs):
    recv_refs = refs[:parts]
    high_ref, low_ref, sums_ref = refs[parts : parts + 3]
    out_ref, wall_ref, values_ref, stress_ref, sems = refs[-5:]
    members, fields, coef, _ = values_ref.shape
    rows = 2 * members
    base = 2 * first
    where = [pl.multiple_of(peer * slots, slots) for peer in peers(parts)]
    b_high, b_low = [
        jnp.concatenate([ref[pl.ds(at, slots), :] for at in where], axis=0)
        for ref in (high_ref, low_ref)
    ]
    scale = lax.rsqrt(sums_ref[base : base + rows] / count + EPSILON)
    copies = []
    for r in range(rows):
        q, f = divmod(r, fields)
        s = jnp.concatenate([ref[pl.ds(r, slots, stride=rows), :] for ref in recv_refs], axis=0)
        s = (s * scale[r : r + 1]).T
        s_high, s_low = split(s)
        o = dot(s_high, b_high, NN) + (dot(s_high, b_low, NN) + dot(s_low, b_high, NN))
        for e in range(2):
            values_ref[2 * q + e, f] = o[e * coef : (e + 1) * coef]
        if f == fields - 1:
            pair = pl.ds(2 * q, 2)
            copies.append(
                pltpu.make_async_copy(
                    values_ref.at[pair], out_ref.at[pl.ds(first + 2 * q, 2)], sems.at[q]
                )
            )
            copies[-1].start()
    me = lax.axis_index("gy")
    near = jnp.bitwise_and(me, 1) != 0
    far = jnp.bitwise_and(me, 2) != 0
    lane = lax.broadcasted_iota(jnp.int32, (rows, LANES), 1)
    tiles = [ref[slots * rows : slots * rows + rows] for ref in recv_refs]
    tiles = [jnp.where(near, tiles[d ^ 1], tiles[d]) for d in range(parts)]
    tiles = [jnp.where(far, tiles[d ^ 2], tiles[d]) * scale for d in range(parts)]
    b_high = high_ref[...]
    b_low = low_ref[...]
    for e in range(2):
        for w in range(2):
            g = jnp.zeros((rows, LANES), jnp.float32)
            for k in range(parts):
                shift = (k * slots - (e * 2 + w) * slots) % LANES
                tile = pltpu.roll(tiles[k], shift, 1) if shift else tiles[k]
                g = jnp.where((lane >= k * slots) & (lane < (k + 1) * slots), tile, g)
            g_high, g_low = split(g)
            o = dot(g_high, b_high, NN) + (dot(g_high, b_low, NN) + dot(g_low, b_high, NN))
            for q in range(members // 2):
                for c in range(2):
                    row = fields * q + 2 * c
                    stress_ref[2 * q + e, w, c : c + 1] = o[row : row + 1]
    copies.append(
        pltpu.make_async_copy(
            stress_ref, wall_ref.at[pl.ds(first, members)], sems.at[members // 2]
        )
    )
    copies[-1].start()
    for copy in copies:
        copy.wait()


def exchanged(pieces, axis):
    n = lax.axis_size(axis)
    got = list(pieces)
    for d in range(n - 1, 0, -1):
        got[d] = lax.ppermute(pieces[d], axis, [(i, i ^ d) for i in range(n)])
    return got


def halo_pairs(n):
    near = [(i, i ^ 1) for i in range(n)]
    far = [(i, (i + (1 if i % 2 else -1)) % n) for i in range(n)]
    return near, far


def axis_hops(n):
    return [1 << i for i in range(n.bit_length() - 1)]


def full_sum(x):
    for axis in ("gy", "gx"):
        n = lax.axis_size(axis)
        for hop in axis_hops(n):
            other = lax.ppermute(x, axis, [(i, i ^ hop) for i in range(n)])
            x = x + other
    return x


SIZES = (4, 4, 4)


def chunks(members):
    sizes = SIZES if sum(SIZES) == members else (2,) * (members // 2)
    return [(sum(sizes[:g]), count) for g, count in enumerate(sizes)]


def per_device(state, inverse):
    members, fields, coef, points = state.shape
    parts = lax.axis_size("gy")
    coef_count = coef * parts
    grid_x = points * lax.axis_size("gx")
    window = points + 2 * HALO
    mine = MODES // parts
    plan = chunks(members)

    values, slopes, back_table = window_tables(window, HALO, points, MODES)
    step_high, step_low = split_table(step_tables(values, slopes, HALO, points))
    back_high, back_low = split_table(back_table)
    k = np.arange(coef_count)
    curvature = k * k / (coef_count * coef_count)
    wall = np.zeros((TILE, coef_count), np.float32)
    wall[0] = curvature
    wall[1] = np.where(k % 2 == 0, -1.0, 1.0) * curvature
    wall = jnp.asarray(wall)

    def call(kernel, vmem, flops, moved, **kwargs):
        return pl.pallas_call(
            kernel,
            compiler_params=pltpu.CompilerParams(vmem_limit_bytes=vmem * MIB),
            cost_estimate=pl.CostEstimate(flops=flops, bytes_accessed=moved, transcendentals=0),
            **kwargs,
        )

    def array(*shape):
        return jax.ShapeDtypeStruct(shape, jnp.float32)

    member_bytes = 4 * fields * coef * points
    packed = []
    for first, count in plan:
        packed.append(
            call(
                functools.partial(pack_kernel, first),
                6,
                10**6,
                2 * count * member_bytes,
                in_specs=[VMEM],
                out_specs=[VMEM] * 2,
                out_shape=[array(count, 2, coef, LANES)] * 2,
            )(state)
        )
    squares = call(
        squares_kernel,
        6,
        10**9,
        10**7,
        in_specs=[VMEM],
        out_specs=VMEM,
        out_shape=array(2 * members, LANES),
    )(state)
    halos = []
    near_pairs, far_pairs = halo_pairs(lax.axis_size("gx"))
    for near, far in packed:
        near = lax.ppermute(near, "gx", near_pairs)
        far = lax.ppermute(far, "gx", far_pairs)
        halos.append((near, far))
    sums = full_sum(squares)

    per_step = 4
    steps = mine // per_step // 2
    split_shape = (per_step, coef_count, coef_count)
    high, low = [], []
    for h in range(2):
        out = call(
            split_kernel,
            8,
            10**7,
            4 * mine * coef_count**2,
            grid=(steps,),
            in_specs=[pl.BlockSpec(split_shape, lambda i, h=h: (h * steps + i, 0, 0))],
            out_specs=[pl.BlockSpec(split_shape, lambda i: (i, 0, 0))] * 2,
            out_shape=[jax.ShapeDtypeStruct((mine // 2,) + split_shape[1:], jnp.bfloat16)] * 2,
        )(inverse)
        high.append(out[0])
        low.append(out[1])

    outputs = []
    for g, (first, count) in enumerate(plan):
        rows = count * fields // 2
        sent = call(
            functools.partial(project_kernel, first),
            8,
            3 * 2 * 2 * (2 * MODES) * (4 * LANES) * count * coef,
            3 * count * member_bytes,
            in_specs=[VMEM] * 5,
            out_specs=[VMEM] * parts,
            out_shape=[array(mine * rows, LANES)] * parts,
        )(state, *halos[g], step_high, step_low)
        got = exchanged(sent, "gy")
        flops = 3 * mine * coef_count**2 * 256
        begun = call(
            functools.partial(begin_kernel, rows),
            6,
            flops,
            2 * mine * coef_count**2,
            in_specs=[VMEM] * 6,
            out_specs=VMEM,
            out_shape=array(mine * 2 * rows, coef_count),
        )(*got[:2], *high, *low)
        solved = call(
            functools.partial(solve_kernel, parts, rows),
            6,
            flops,
            2 * mine * coef_count**2,
            in_specs=[VMEM] * 8,
            out_specs=[VMEM] * parts,
            out_shape=[array((mine + 1) * rows + -(mine + 1) * rows % TILE, LANES)] * parts,
        )(*got[2:], *high, *low, begun, wall)
        returned = exchanged(solved, "gy")

        outputs = call(
            functools.partial(
                back_kernel, float(fields * coef_count * grid_x), first, mine, parts
            ),
            8,
            3 * 2 * MODES * points * count * fields * coef,
            2 * count * member_bytes,
            in_specs=[VMEM] * (parts + 3) + [ANY] * len(outputs),
            out_specs=[ANY] * 2,
            out_shape=[array(*state.shape), array(members, 2, 2, points)],
            scratch_shapes=[
                pltpu.VMEM((count, fields, coef, points), jnp.float32),
                pltpu.VMEM((count, 2, 2, points), jnp.float32),
                pltpu.SemaphoreType.DMA((count // 2 + 1,)),
            ],
            input_output_aliases={parts + 3 + i: i for i in range(len(outputs))},
        )(*returned, back_high, back_low, sums, *outputs)
    return tuple(outputs)


def solution(mesh):
    placed = (P(None, None, "gy", "gx"), P("gy", None, None))

    return jax.shard_map(
        per_device,
        mesh=mesh,
        in_specs=placed,
        out_specs=(P(None, None, "gy", "gx"), P(None, None, None, "gx")),
        check_vma=False,
    )
```

```python
import functools
import math

import jax
import jax.numpy as jnp
import numpy as np
from jax import lax
from jax.experimental import pallas as pl
from jax.experimental.pallas import tpu as pltpu
from jax.sharding import PartitionSpec as P


MODES = 128
HALO = 64

EPSILON = 1e-06
TIME_STEP = 0.5
MEAN_FLOW = 0.8
CORIOLIS = 0.6
STRATIFICATION = 0.9

LANES = 128
MIB = 1 << 20
TILE = 8
VMEM = pl.BlockSpec(memory_space=pltpu.VMEM)
ANY = pl.BlockSpec(memory_space=pl.ANY)
NT = (((1,), (1,)), ((), ()))
NN = (((1,), (0,)), ((), ()))
TN = (((0,), (0,)), ((), ()))


def window_tables(window, rim_width, points, mode_count):
    position = np.arange(window)
    mode_index = np.arange(mode_count)
    half_count = mode_count // 2
    is_cosine = mode_index <= half_count
    wave_index = np.where(is_cosine, mode_index, mode_index - half_count)
    product_index = position[:, None] * wave_index[None, :] % window
    phases = 2.0 * np.pi * product_index / window
    weights_norm = np.where(wave_index == 0, np.sqrt(1.0 / window), np.sqrt(2.0 / window))
    basis = np.where(is_cosine[None, :], np.cos(phases), np.sin(phases)) * weights_norm[None, :]
    wavenumber = 2.0 * np.pi * wave_index / window
    paired = wave_index[:, None] == wave_index[None, :]
    to_sine = is_cosine[:, None] & ~is_cosine[None, :] & paired
    to_cosine = ~is_cosine[:, None] & is_cosine[None, :] & paired
    derivative = np.where(to_sine, -wavenumber[:, None], 0.0) + np.where(
        to_cosine, wavenumber[:, None], 0.0
    )
    taper = 0.25 + 0.75 * np.sin(np.pi * (position + 0.5) / window) ** 2
    values = basis * taper[:, None]
    slopes = (basis @ derivative) * taper[:, None]
    back_table = (
        basis[rim_width : rim_width + points, :] / taper[rim_width : rim_width + points, None]
    ).T
    return values, slopes, back_table


def step_tables(values, slopes, rim, points):
    direct = values - TIME_STEP * MEAN_FLOW * slopes
    couplings = (
        (TIME_STEP * CORIOLIS, -TIME_STEP * CORIOLIS),
        (TIME_STEP, -TIME_STEP * STRATIFICATION),
    )
    tables = []
    for to_first, to_second in couplings:
        first = (direct, to_first * values)
        second = (to_second * values, direct)
        rows = []
        for part in (first, second):
            pieces = []
            for begin, end in ((rim, rim + points), (0, rim), (rim + points, points + 2 * rim)):
                pieces += [part[0][begin:end].T, part[1][begin:end].T]
            rows.append(np.concatenate(pieces, axis=1))
        tables.append(np.concatenate(rows, axis=0))
    return np.stack(tables)


def split_table(table):
    table = np.asarray(table, np.float32)
    high = table.astype(jnp.bfloat16)
    low = (table - high.astype(np.float32)).astype(jnp.bfloat16)
    return jnp.asarray(high), jnp.asarray(low)


def split(x):
    high = x.astype(jnp.bfloat16)
    low = (x - high.astype(jnp.float32)).astype(jnp.bfloat16)
    return high, low


def dot(a, b, dims):
    return lax.dot_general(a, b, dims, preferred_element_type=jnp.float32)


def left_lanes(shape):
    return lax.broadcasted_iota(jnp.int32, shape, len(shape) - 1) < LANES // 2


def swap(x):
    return pltpu.roll(x, LANES // 2, len(x.shape) - 1)


def pack_kernel(base, state_ref, near_ref, far_ref):
    rows = state_ref.shape[2]
    even = jnp.bitwise_and(lax.axis_index("gx"), 1) == 0
    left = left_lanes((rows, LANES))
    for e in range(near_ref.shape[0]):
        for p in range(2):
            a = state_ref[base + e, p]
            b = state_ref[base + e, p + 2]
            last = jnp.where(left, swap(a), b)
            first = jnp.where(left, a, swap(b))
            near_ref[e, p] = jnp.where(even, last, first)
            far_ref[e, p] = jnp.where(even, first, last)


def squares_kernel(state_ref, sums_ref):
    members, fields, rows, _ = state_ref.shape
    half = left_lanes((fields, LANES))
    for q in range(members // 2):
        totals = []
        for e in range(2):
            acc = jnp.zeros((rows, LANES), jnp.float32)
            for f in range(fields):
                a = state_ref[2 * q + e, f]
                acc += a * a
            totals.append(jnp.sum(acc))
        sums_ref[fields * q : fields * (q + 1)] = jnp.where(half, totals[0], totals[1])


def peers(parts):
    me = lax.axis_index("gy")
    return [jnp.bitwise_xor(me, d) for d in range(parts)]


def reorder_lanes(x):
    me = lax.axis_index("gy")
    far = jnp.bitwise_and(me, 2) != 0
    near = jnp.bitwise_and(me, 1) != 0
    a, b = x[..., :LANES], x[..., LANES:]
    a, b = jnp.where(far, b, a), jnp.where(far, a, b)
    return jnp.where(near, swap(a), a), jnp.where(near, swap(b), b)


def split_kernel(inverse_ref, high_ref, low_ref):
    coef_count = inverse_ref.shape[1]
    coef = LANES // 2
    for d, peer in enumerate(peers(coef_count // coef)):
        rows = pl.ds(pl.multiple_of(peer * coef, coef), coef)
        for h, x in enumerate(reorder_lanes(inverse_ref[:, rows, :])):
            at = (slice(None), slice(d * coef, (d + 1) * coef), slice(h * LANES, (h + 1) * LANES))
            high_ref[at], low_ref[at] = split(x)


def project_kernel(base, state_ref, near_ref, far_ref, high_ref, low_ref, *out_refs):
    parts = len(out_refs)
    members, _, coef, _ = near_ref.shape
    rows = 2 * members
    slots = out_refs[0].shape[0] // rows
    count = slots * parts
    lane = lax.broadcasted_iota(jnp.int32, (1, members * coef), 1)
    index = lax.axis_index("gy") * coef + lax.rem(lane, coef)
    interior = index < coef * parts - 2
    even = jnp.bitwise_and(lax.axis_index("gx"), 1) == 0
    where = [pl.multiple_of(peer * slots, slots) for peer in peers(parts)]
    for p in range(2):
        near = near_ref[:, p].reshape(members * coef, LANES)
        far = far_ref[:, p].reshape(members * coef, LANES)
        x = jnp.concatenate(
            [
                state_ref[base : base + members, p].reshape(members * coef, LANES),
                state_ref[base : base + members, p + 2].reshape(members * coef, LANES),
                jnp.where(even, far, near),
                jnp.where(even, near, far),
            ],
            axis=1,
        )
        x_high, x_low = split(x)
        w_high, w_low = [
            jnp.concatenate(
                [ref[p, pl.ds(f * count + at, slots), :] for f in range(2) for at in where], axis=0
            )
            for ref in (high_ref, low_ref)
        ]
        t = dot(w_high, x_high, NT) + (dot(w_high, x_low, NT) + dot(w_low, x_high, NT))
        t = jnp.where(interior, t, 0.0)
        for d in range(parts):
            for f in range(2):
                first = f * count + d * slots
                for q in range(members // 2):
                    out_refs[d][pl.ds(4 * q + p + 2 * f, slots, stride=rows), :] = t[
                        first : first + slots, q * LANES : (q + 1) * LANES
                    ]


def products(i, h, rows, modes, recv_refs, high_refs, low_refs):
    unit = rows * modes
    left = left_lanes((unit, LANES))
    a, b = [ref[i * unit : (i + 1) * unit] for ref in recv_refs]
    even = jnp.where(left, a, swap(b))
    odd = jnp.where(left, swap(a), b)
    columns = slice(h * LANES, (h + 1) * LANES)
    found = []
    for j in range(modes):
        r = jnp.concatenate([x[j * rows : (j + 1) * rows] for x in (even, odd)], axis=0)
        half, at = divmod(i * modes + j, high_refs[0].shape[0])
        v_high = high_refs[half][at, :, columns]
        v_low = low_refs[half][at, :, columns]
        r_high, r_low = split(r)
        both = dot(jnp.concatenate([r_high, r_low], axis=0), v_high, NT)
        found.append(both[: 2 * rows] + (both[2 * rows :] + dot(r_high, v_low, NT)))
    return found


def begin_kernel(rows, *refs):
    recv_refs, high_refs, low_refs, out_ref = refs[:2], refs[2:4], refs[4:6], refs[6]
    modes = TILE // math.gcd(rows, TILE)
    for i in range(recv_refs[0].shape[0] // (rows * modes)):
        for j, o in enumerate(products(i, 0, rows, modes, recv_refs, high_refs, low_refs)):
            m = i * modes + j
            out_ref[m * 2 * rows : (m + 1) * 2 * rows] = o


def solve_kernel(parts, rows, *refs):
    recv_refs, high_refs, low_refs = refs[:2], refs[2:4], refs[4:6]
    begun_ref, wall_ref = refs[6:8]
    out_refs = refs[8:]
    slots = recv_refs[0].shape[0] // rows
    modes = TILE // math.gcd(rows, TILE)
    unit = rows * modes
    left = left_lanes((unit, LANES))
    lane = lax.broadcasted_iota(jnp.int32, (unit, LANES), 1)
    mode = lax.broadcasted_iota(jnp.int32, (unit, LANES), 0) // rows
    wall = jnp.concatenate(reorder_lanes(wall_ref[...]), axis=1)
    sums = jnp.zeros((unit, LANES), jnp.float32)
    for i in range(slots // modes):
        tile = slice(i * unit, (i + 1) * unit)
        solved = []
        for j, o in enumerate(products(i, 1, rows, modes, recv_refs, high_refs, low_refs)):
            m = i * modes + j
            solved.append(o + begun_ref[m * 2 * rows : (m + 1) * 2 * rows])
        even = jnp.concatenate([o[:rows] for o in solved], axis=0)
        odd = jnp.concatenate([o[rows:] for o in solved], axis=0)
        for d in range(0, parts, 2):
            a = even[:, d * LANES // 2 : d * LANES // 2 + LANES]
            b = odd[:, d * LANES // 2 : d * LANES // 2 + LANES]
            out_refs[d][tile] = jnp.where(left, a, swap(b))
            out_refs[d + 1][tile] = jnp.where(left, swap(a), b)
        for e, o in enumerate((even, odd)):
            for w in range(2):
                q = jnp.sum(o * wall[w : w + 1], axis=1, keepdims=True)
                sums = jnp.where(lane == (2 * e + w) * slots + i * modes + mode, q, sums)
    total = sums[:rows]
    for j in range(1, modes):
        total = total + sums[j * rows : (j + 1) * rows]
    for ref in out_refs:
        ref[slots * rows : slots * rows + rows] = total
        if rows % TILE:
            spare = ref.shape[0] - (slots + 1) * rows
            ref[(slots + 1) * rows :] = jnp.zeros((spare, LANES), jnp.float32)


def back_kernel(count, first, slots, parts, *refs):
    recv_refs = refs[:parts]
    high_ref, low_ref, sums_ref = refs[parts : parts + 3]
    out_ref, wall_ref, values_ref, stress_ref, sems = refs[-5:]
    members, fields, coef, _ = values_ref.shape
    rows = 2 * members
    base = 2 * first
    where = [pl.multiple_of(peer * slots, slots) for peer in peers(parts)]
    b_high, b_low = [
        jnp.concatenate([ref[pl.ds(at, slots), :] for at in where], axis=0)
        for ref in (high_ref, low_ref)
    ]
    scale = lax.rsqrt(sums_ref[base : base + rows] / count + EPSILON)
    copies = []
    for r in range(rows):
        q, f = divmod(r, fields)
        s = jnp.concatenate([ref[pl.ds(r, slots, stride=rows), :] for ref in recv_refs], axis=0)
        s_high, s_low = split(s * scale[r : r + 1])
        o = dot(s_high, b_high, TN) + (dot(s_high, b_low, TN) + dot(s_low, b_high, TN))
        for e in range(2):
            values_ref[2 * q + e, f] = o[e * coef : (e + 1) * coef]
        if f == fields - 1:
            pair = pl.ds(2 * q, 2)
            copies.append(
                pltpu.make_async_copy(
                    values_ref.at[pair], out_ref.at[pl.ds(first + 2 * q, 2)], sems.at[q]
                )
            )
            copies[-1].start()
    me = lax.axis_index("gy")
    near = jnp.bitwise_and(me, 1) != 0
    far = jnp.bitwise_and(me, 2) != 0
    lane = lax.broadcasted_iota(jnp.int32, (rows, LANES), 1)
    tiles = [ref[slots * rows : slots * rows + rows] for ref in recv_refs]
    tiles = [jnp.where(near, tiles[d ^ 1], tiles[d]) for d in range(parts)]
    tiles = [jnp.where(far, tiles[d ^ 2], tiles[d]) * scale for d in range(parts)]
    b_high = high_ref[...]
    b_low = low_ref[...]
    for e in range(2):
        for w in range(2):
            g = jnp.zeros((rows, LANES), jnp.float32)
            for k in range(parts):
                shift = (k * slots - (e * 2 + w) * slots) % LANES
                tile = pltpu.roll(tiles[k], shift, 1) if shift else tiles[k]
                g = jnp.where((lane >= k * slots) & (lane < (k + 1) * slots), tile, g)
            g_high, g_low = split(g)
            o = dot(g_high, b_high, NN) + (dot(g_high, b_low, NN) + dot(g_low, b_high, NN))
            for q in range(members // 2):
                for c in range(2):
                    row = fields * q + 2 * c
                    stress_ref[2 * q + e, w, c : c + 1] = o[row : row + 1]
    copies.append(
        pltpu.make_async_copy(
            stress_ref, wall_ref.at[pl.ds(first, members)], sems.at[members // 2]
        )
    )
    copies[-1].start()
    for copy in copies:
        copy.wait()


def exchanged(pieces, axis):
    n = lax.axis_size(axis)
    got = list(pieces)
    for d in range(n - 1, 0, -1):
        got[d] = lax.ppermute(pieces[d], axis, [(i, i ^ d) for i in range(n)])
    return got


def halo_pairs(n):
    near = [(i, i ^ 1) for i in range(n)]
    far = [(i, (i + (1 if i % 2 else -1)) % n) for i in range(n)]
    return near, far


def axis_hops(n):
    return [1 << i for i in range(n.bit_length() - 1)]


def full_sum(x):
    for axis in ("gy", "gx"):
        n = lax.axis_size(axis)
        for hop in axis_hops(n):
            other = lax.ppermute(x, axis, [(i, i ^ hop) for i in range(n)])
            x = x + other
    return x


SIZES = (4, 4, 4)


def chunks(members):
    sizes = SIZES if sum(SIZES) == members else (2,) * (members // 2)
    return [(sum(sizes[:g]), count) for g, count in enumerate(sizes)]


def per_device(state, inverse):
    members, fields, coef, points = state.shape
    parts = lax.axis_size("gy")
    coef_count = coef * parts
    grid_x = points * lax.axis_size("gx")
    window = points + 2 * HALO
    mine = MODES // parts
    plan = chunks(members)

    values, slopes, back_table = window_tables(window, HALO, points, MODES)
    step_high, step_low = split_table(step_tables(values, slopes, HALO, points))
    back_high, back_low = split_table(back_table)
    k = np.arange(coef_count)
    curvature = k * k / (coef_count * coef_count)
    wall = np.zeros((TILE, coef_count), np.float32)
    wall[0] = curvature
    wall[1] = np.where(k % 2 == 0, -1.0, 1.0) * curvature
    wall = jnp.asarray(wall)

    def call(kernel, vmem, flops, moved, **kwargs):
        return pl.pallas_call(
            kernel,
            compiler_params=pltpu.CompilerParams(vmem_limit_bytes=vmem * MIB),
            cost_estimate=pl.CostEstimate(flops=flops, bytes_accessed=moved, transcendentals=0),
            **kwargs,
        )

    def array(*shape):
        return jax.ShapeDtypeStruct(shape, jnp.float32)

    member_bytes = 4 * fields * coef * points
    packed = []
    for first, count in plan:
        packed.append(
            call(
                functools.partial(pack_kernel, first),
                6,
                10**6,
                2 * count * member_bytes,
                in_specs=[VMEM],
                out_specs=[VMEM] * 2,
                out_shape=[array(count, 2, coef, LANES)] * 2,
            )(state)
        )
    squares = call(
        squares_kernel,
        6,
        10**9,
        10**7,
        in_specs=[VMEM],
        out_specs=VMEM,
        out_shape=array(2 * members, LANES),
    )(state)
    halos = []
    near_pairs, far_pairs = halo_pairs(lax.axis_size("gx"))
    for near, far in packed:
        near = lax.ppermute(near, "gx", near_pairs)
        far = lax.ppermute(far, "gx", far_pairs)
        halos.append((near, far))
    sums = full_sum(squares)

    per_step = 4
    steps = mine // per_step // 2
    split_shape = (per_step, coef_count, coef_count)
    high, low = [], []
    for h in range(2):
        out = call(
            split_kernel,
            8,
            10**7,
            4 * mine * coef_count**2,
            grid=(steps,),
            in_specs=[pl.BlockSpec(split_shape, lambda i, h=h: (h * steps + i, 0, 0))],
            out_specs=[pl.BlockSpec(split_shape, lambda i: (i, 0, 0))] * 2,
            out_shape=[jax.ShapeDtypeStruct((mine // 2,) + split_shape[1:], jnp.bfloat16)] * 2,
        )(inverse)
        high.append(out[0])
        low.append(out[1])

    outputs = []
    for g, (first, count) in enumerate(plan):
        rows = count * fields // 2
        sent = call(
            functools.partial(project_kernel, first),
            8,
            3 * 2 * 2 * (2 * MODES) * (4 * LANES) * count * coef,
            3 * count * member_bytes,
            in_specs=[VMEM] * 5,
            out_specs=[VMEM] * parts,
            out_shape=[array(mine * rows, LANES)] * parts,
        )(state, *halos[g], step_high, step_low)
        got = exchanged(sent, "gy")
        flops = 3 * mine * coef_count**2 * 256
        begun = call(
            functools.partial(begin_kernel, rows),
            6,
            flops,
            2 * mine * coef_count**2,
            in_specs=[VMEM] * 6,
            out_specs=VMEM,
            out_shape=array(mine * 2 * rows, coef_count),
        )(*got[:2], *high, *low)
        solved = call(
            functools.partial(solve_kernel, parts, rows),
            6,
            flops,
            2 * mine * coef_count**2,
            in_specs=[VMEM] * 8,
            out_specs=[VMEM] * parts,
            out_shape=[array((mine + 1) * rows + -(mine + 1) * rows % TILE, LANES)] * parts,
        )(*got[2:], *high, *low, begun, wall)
        returned = exchanged(solved, "gy")

        outputs = call(
            functools.partial(
                back_kernel, float(fields * coef_count * grid_x), first, mine, parts
            ),
            8,
            3 * 2 * MODES * points * count * fields * coef,
            2 * count * member_bytes,
            in_specs=[VMEM] * (parts + 3) + [ANY] * len(outputs),
            out_specs=[ANY] * 2,
            out_shape=[array(*state.shape), array(members, 2, 2, points)],
            scratch_shapes=[
                pltpu.VMEM((count, fields, coef, points), jnp.float32),
                pltpu.VMEM((count, 2, 2, points), jnp.float32),
                pltpu.SemaphoreType.DMA((count // 2 + 1,)),
            ],
            input_output_aliases={parts + 3 + i: i for i in range(len(outputs))},
        )(*returned, back_high, back_low, sums, *outputs)
    return tuple(outputs)


def solution(mesh):
    placed = (P(None, None, "gy", "gx"), P("gy", None, None))

    return jax.shard_map(
        per_device,
        mesh=mesh,
        in_specs=placed,
        out_specs=(P(None, None, "gy", "gx"), P(None, None, None, "gx")),
        check_vma=False,
    )
```

```python
import functools
import math

import jax
import jax.numpy as jnp
import numpy as np
from jax import lax
from jax.experimental import pallas as pl
from jax.experimental.pallas import tpu as pltpu
from jax.sharding import PartitionSpec as P


MODES = 128
HALO = 64

EPSILON = 1e-06
TIME_STEP = 0.5
MEAN_FLOW = 0.8
CORIOLIS = 0.6
STRATIFICATION = 0.9

LANES = 128
MIB = 1 << 20
TILE = 8
VMEM = pl.BlockSpec(memory_space=pltpu.VMEM)
ANY = pl.BlockSpec(memory_space=pl.ANY)
NT = (((1,), (1,)), ((), ()))
NN = (((1,), (0,)), ((), ()))
TN = (((0,), (0,)), ((), ()))


def window_tables(window, rim_width, points, mode_count):
    position = np.arange(window)
    mode_index = np.arange(mode_count)
    half_count = mode_count // 2
    is_cosine = mode_index <= half_count
    wave_index = np.where(is_cosine, mode_index, mode_index - half_count)
    product_index = position[:, None] * wave_index[None, :] % window
    phases = 2.0 * np.pi * product_index / window
    weights_norm = np.where(wave_index == 0, np.sqrt(1.0 / window), np.sqrt(2.0 / window))
    basis = np.where(is_cosine[None, :], np.cos(phases), np.sin(phases)) * weights_norm[None, :]
    wavenumber = 2.0 * np.pi * wave_index / window
    paired = wave_index[:, None] == wave_index[None, :]
    to_sine = is_cosine[:, None] & ~is_cosine[None, :] & paired
    to_cosine = ~is_cosine[:, None] & is_cosine[None, :] & paired
    derivative = np.where(to_sine, -wavenumber[:, None], 0.0) + np.where(
        to_cosine, wavenumber[:, None], 0.0
    )
    taper = 0.25 + 0.75 * np.sin(np.pi * (position + 0.5) / window) ** 2
    values = basis * taper[:, None]
    slopes = (basis @ derivative) * taper[:, None]
    back_table = (
        basis[rim_width : rim_width + points, :] / taper[rim_width : rim_width + points, None]
    ).T
    return values, slopes, back_table


def step_tables(values, slopes, rim, points):
    direct = values - TIME_STEP * MEAN_FLOW * slopes
    couplings = (
        (TIME_STEP * CORIOLIS, -TIME_STEP * CORIOLIS),
        (TIME_STEP, -TIME_STEP * STRATIFICATION),
    )
    tables = []
    for to_first, to_second in couplings:
        first = (direct, to_first * values)
        second = (to_second * values, direct)
        rows = []
        for part in (first, second):
            pieces = []
            for begin, end in ((rim, rim + points), (0, rim), (rim + points, points + 2 * rim)):
                pieces += [part[0][begin:end].T, part[1][begin:end].T]
            rows.append(np.concatenate(pieces, axis=1))
        tables.append(np.concatenate(rows, axis=0))
    return np.stack(tables)


def split_table(table):
    table = np.asarray(table, np.float32)
    high = table.astype(jnp.bfloat16)
    low = (table - high.astype(np.float32)).astype(jnp.bfloat16)
    return jnp.asarray(high), jnp.asarray(low)


def split(x):
    high = x.astype(jnp.bfloat16)
    low = (x - high.astype(jnp.float32)).astype(jnp.bfloat16)
    return high, low


def dot(a, b, dims):
    return lax.dot_general(a, b, dims, preferred_element_type=jnp.float32)


def left_lanes(shape):
    return lax.broadcasted_iota(jnp.int32, shape, len(shape) - 1) < LANES // 2


def swap(x):
    return pltpu.roll(x, LANES // 2, len(x.shape) - 1)


def pack_kernel(base, state_ref, near_ref, far_ref):
    rows = state_ref.shape[2]
    even = jnp.bitwise_and(lax.axis_index("gx"), 1) == 0
    left = left_lanes((rows, LANES))
    for e in range(near_ref.shape[0]):
        for p in range(2):
            a = state_ref[base + e, p]
            b = state_ref[base + e, p + 2]
            last = jnp.where(left, swap(a), b)
            first = jnp.where(left, a, swap(b))
            near_ref[e, p] = jnp.where(even, last, first)
            far_ref[e, p] = jnp.where(even, first, last)


def squares_kernel(state_ref, sums_ref):
    members, fields, rows, _ = state_ref.shape
    half = left_lanes((fields, LANES))
    for q in range(members // 2):
        totals = []
        for e in range(2):
            acc = jnp.zeros((rows, LANES), jnp.float32)
            for f in range(fields):
                a = state_ref[2 * q + e, f]
                acc += a * a
            totals.append(jnp.sum(acc))
        sums_ref[fields * q : fields * (q + 1)] = jnp.where(half, totals[0], totals[1])


def peers(parts):
    me = lax.axis_index("gy")
    return [jnp.bitwise_xor(me, d) for d in range(parts)]


def reorder_lanes(x):
    me = lax.axis_index("gy")
    far = jnp.bitwise_and(me, 2) != 0
    near = jnp.bitwise_and(me, 1) != 0
    a, b = x[..., :LANES], x[..., LANES:]
    a, b = jnp.where(far, b, a), jnp.where(far, a, b)
    return jnp.where(near, swap(a), a), jnp.where(near, swap(b), b)


def split_kernel(inverse_ref, high_ref, low_ref):
    coef_count = inverse_ref.shape[1]
    coef = LANES // 2
    for d, peer in enumerate(peers(coef_count // coef)):
        rows = pl.ds(pl.multiple_of(peer * coef, coef), coef)
        for h, x in enumerate(reorder_lanes(inverse_ref[:, rows, :])):
            at = (slice(None), slice(d * coef, (d + 1) * coef), slice(h * LANES, (h + 1) * LANES))
            high_ref[at], low_ref[at] = split(x)


def table_rows(ref, p, where, count, slots, columns):
    return jnp.concatenate(
        [ref[p, pl.ds(f * count + at, slots), columns] for f in range(2) for at in where], axis=0
    )


def own_kernel(base, parts, state_ref, high_ref, low_ref, out_ref):
    coef = state_ref.shape[2]
    members = out_ref.shape[2] // coef
    count = high_ref.shape[1] // 2
    slots = count // parts
    where = [pl.multiple_of(peer * slots, slots) for peer in peers(parts)]
    columns = slice(0, 2 * LANES)
    for p in range(2):
        x = jnp.concatenate(
            [
                state_ref[base : base + members, p].reshape(members * coef, LANES),
                state_ref[base : base + members, p + 2].reshape(members * coef, LANES),
            ],
            axis=1,
        )
        x_high, x_low = split(x)
        w_high = table_rows(high_ref, p, where, count, slots, columns)
        w_low = table_rows(low_ref, p, where, count, slots, columns)
        out_ref[p] = dot(w_high, x_high, NT) + (dot(w_high, x_low, NT) + dot(w_low, x_high, NT))


def project_kernel(own_ref, near_ref, far_ref, high_ref, low_ref, *out_refs):
    parts = len(out_refs)
    members, _, coef, _ = near_ref.shape
    rows = 2 * members
    slots = out_refs[0].shape[0] // rows
    count = slots * parts
    lane = lax.broadcasted_iota(jnp.int32, (1, members * coef), 1)
    index = lax.axis_index("gy") * coef + lax.rem(lane, coef)
    interior = index < coef * parts - 2
    even = jnp.bitwise_and(lax.axis_index("gx"), 1) == 0
    where = [pl.multiple_of(peer * slots, slots) for peer in peers(parts)]
    for p in range(2):
        near = near_ref[:, p].reshape(members * coef, LANES)
        far = far_ref[:, p].reshape(members * coef, LANES)
        x = jnp.concatenate(
            [
                jnp.where(even, far, near),
                jnp.where(even, near, far),
            ],
            axis=1,
        )
        x_high, x_low = split(x)
        w_high = table_rows(high_ref, p, where, count, slots, slice(2 * LANES, 4 * LANES))
        w_low = table_rows(low_ref, p, where, count, slots, slice(2 * LANES, 4 * LANES))
        t = dot(w_high, x_high, NT) + (dot(w_high, x_low, NT) + dot(w_low, x_high, NT))
        t = jnp.where(interior, t + own_ref[p], 0.0)
        for d in range(parts):
            for f in range(2):
                first = f * count + d * slots
                for q in range(members // 2):
                    out_refs[d][pl.ds(4 * q + p + 2 * f, slots, stride=rows), :] = t[
                        first : first + slots, q * LANES : (q + 1) * LANES
                    ]


def products(i, h, rows, modes, recv_refs, high_refs, low_refs):
    unit = rows * modes
    left = left_lanes((unit, LANES))
    a, b = [ref[i * unit : (i + 1) * unit] for ref in recv_refs]
    even = jnp.where(left, a, swap(b))
    odd = jnp.where(left, swap(a), b)
    columns = slice(h * LANES, (h + 1) * LANES)
    found = []
    for j in range(modes):
        r = jnp.concatenate([x[j * rows : (j + 1) * rows] for x in (even, odd)], axis=0)
        half, at = divmod(i * modes + j, high_refs[0].shape[0])
        v_high = high_refs[half][at, :, columns]
        v_low = low_refs[half][at, :, columns]
        r_high, r_low = split(r)
        both = dot(jnp.concatenate([r_high, r_low], axis=0), v_high, NT)
        found.append(both[: 2 * rows] + (both[2 * rows :] + dot(r_high, v_low, NT)))
    return found


def begin_kernel(rows, *refs):
    recv_refs, high_refs, low_refs, out_ref = refs[:2], refs[2:4], refs[4:6], refs[6]
    modes = TILE // math.gcd(rows, TILE)
    for i in range(recv_refs[0].shape[0] // (rows * modes)):
        for j, o in enumerate(products(i, 0, rows, modes, recv_refs, high_refs, low_refs)):
            m = i * modes + j
            out_ref[m * 2 * rows : (m + 1) * 2 * rows] = o


def solve_kernel(parts, rows, *refs):
    recv_refs, high_refs, low_refs = refs[:2], refs[2:4], refs[4:6]
    begun_ref, wall_ref = refs[6:8]
    out_refs = refs[8:]
    slots = recv_refs[0].shape[0] // rows
    modes = TILE // math.gcd(rows, TILE)
    unit = rows * modes
    left = left_lanes((unit, LANES))
    lane = lax.broadcasted_iota(jnp.int32, (unit, LANES), 1)
    mode = lax.broadcasted_iota(jnp.int32, (unit, LANES), 0) // rows
    wall = jnp.concatenate(reorder_lanes(wall_ref[...]), axis=1)
    sums = jnp.zeros((unit, LANES), jnp.float32)
    for i in range(slots // modes):
        tile = slice(i * unit, (i + 1) * unit)
        solved = []
        for j, o in enumerate(products(i, 1, rows, modes, recv_refs, high_refs, low_refs)):
            m = i * modes + j
            solved.append(o + begun_ref[m * 2 * rows : (m + 1) * 2 * rows])
        even = jnp.concatenate([o[:rows] for o in solved], axis=0)
        odd = jnp.concatenate([o[rows:] for o in solved], axis=0)
        for d in range(0, parts, 2):
            a = even[:, d * LANES // 2 : d * LANES // 2 + LANES]
            b = odd[:, d * LANES // 2 : d * LANES // 2 + LANES]
            out_refs[d][tile] = jnp.where(left, a, swap(b))
            out_refs[d + 1][tile] = jnp.where(left, swap(a), b)
        for e, o in enumerate((even, odd)):
            for w in range(2):
                q = jnp.sum(o * wall[w : w + 1], axis=1, keepdims=True)
                sums = jnp.where(lane == (2 * e + w) * slots + i * modes + mode, q, sums)
    total = sums[:rows]
    for j in range(1, modes):
        total = total + sums[j * rows : (j + 1) * rows]
    for ref in out_refs:
        ref[slots * rows : slots * rows + rows] = total
        if rows % TILE:
            spare = ref.shape[0] - (slots + 1) * rows
            ref[(slots + 1) * rows :] = jnp.zeros((spare, LANES), jnp.float32)


def back_kernel(count, first, slots, parts, *refs):
    recv_refs = refs[:parts]
    high_ref, low_ref, sums_ref = refs[parts : parts + 3]
    out_ref, wall_ref, values_ref, stress_ref, sems = refs[-5:]
    members, fields, coef, _ = values_ref.shape
    rows = 2 * members
    base = 2 * first
    where = [pl.multiple_of(peer * slots, slots) for peer in peers(parts)]
    b_high, b_low = [
        jnp.concatenate([ref[pl.ds(at, slots), :] for at in where], axis=0)
        for ref in (high_ref, low_ref)
    ]
    scale = lax.rsqrt(sums_ref[base : base + rows] / count + EPSILON)
    copies = []
    for r in range(rows):
        q, f = divmod(r, fields)
        s = jnp.concatenate([ref[pl.ds(r, slots, stride=rows), :] for ref in recv_refs], axis=0)
        s_high, s_low = split(s * scale[r : r + 1])
        o = dot(s_high, b_high, TN) + (dot(s_high, b_low, TN) + dot(s_low, b_high, TN))
        for e in range(2):
            values_ref[2 * q + e, f] = o[e * coef : (e + 1) * coef]
        if f == fields - 1:
            pair = pl.ds(2 * q, 2)
            copies.append(
                pltpu.make_async_copy(
                    values_ref.at[pair], out_ref.at[pl.ds(first + 2 * q, 2)], sems.at[q]
                )
            )
            copies[-1].start()
    me = lax.axis_index("gy")
    near = jnp.bitwise_and(me, 1) != 0
    far = jnp.bitwise_and(me, 2) != 0
    lane = lax.broadcasted_iota(jnp.int32, (rows, LANES), 1)
    tiles = [ref[slots * rows : slots * rows + rows] for ref in recv_refs]
    tiles = [jnp.where(near, tiles[d ^ 1], tiles[d]) for d in range(parts)]
    tiles = [jnp.where(far, tiles[d ^ 2], tiles[d]) * scale for d in range(parts)]
    b_high = high_ref[...]
    b_low = low_ref[...]
    for e in range(2):
        for w in range(2):
            g = jnp.zeros((rows, LANES), jnp.float32)
            for k in range(parts):
                shift = (k * slots - (e * 2 + w) * slots) % LANES
                tile = pltpu.roll(tiles[k], shift, 1) if shift else tiles[k]
                g = jnp.where((lane >= k * slots) & (lane < (k + 1) * slots), tile, g)
            g_high, g_low = split(g)
            o = dot(g_high, b_high, NN) + (dot(g_high, b_low, NN) + dot(g_low, b_high, NN))
            for q in range(members // 2):
                for c in range(2):
                    row = fields * q + 2 * c
                    stress_ref[2 * q + e, w, c : c + 1] = o[row : row + 1]
    copies.append(
        pltpu.make_async_copy(
            stress_ref, wall_ref.at[pl.ds(first, members)], sems.at[members // 2]
        )
    )
    copies[-1].start()
    for copy in copies:
        copy.wait()


def exchanged(pieces, axis):
    n = lax.axis_size(axis)
    got = list(pieces)
    for d in range(n - 1, 0, -1):
        got[d] = lax.ppermute(pieces[d], axis, [(i, i ^ d) for i in range(n)])
    return got


def halo_pairs(n):
    near = [(i, i ^ 1) for i in range(n)]
    far = [(i, (i + (1 if i % 2 else -1)) % n) for i in range(n)]
    return near, far


def axis_hops(n):
    return [1 << i for i in range(n.bit_length() - 1)]


def full_sum(x):
    for axis in ("gy", "gx"):
        n = lax.axis_size(axis)
        for hop in axis_hops(n):
            other = lax.ppermute(x, axis, [(i, i ^ hop) for i in range(n)])
            x = x + other
    return x


SIZES = (4, 4, 4)


def chunks(members):
    sizes = SIZES if sum(SIZES) == members else (2,) * (members // 2)
    return [(sum(sizes[:g]), count) for g, count in enumerate(sizes)]


def per_device(state, inverse):
    members, fields, coef, points = state.shape
    parts = lax.axis_size("gy")
    coef_count = coef * parts
    grid_x = points * lax.axis_size("gx")
    window = points + 2 * HALO
    mine = MODES // parts
    plan = chunks(members)

    values, slopes, back_table = window_tables(window, HALO, points, MODES)
    step_high, step_low = split_table(step_tables(values, slopes, HALO, points))
    back_high, back_low = split_table(back_table)
    k = np.arange(coef_count)
    curvature = k * k / (coef_count * coef_count)
    wall = np.zeros((TILE, coef_count), np.float32)
    wall[0] = curvature
    wall[1] = np.where(k % 2 == 0, -1.0, 1.0) * curvature
    wall = jnp.asarray(wall)

    def call(kernel, vmem, flops, moved, **kwargs):
        return pl.pallas_call(
            kernel,
            compiler_params=pltpu.CompilerParams(vmem_limit_bytes=vmem * MIB),
            cost_estimate=pl.CostEstimate(flops=flops, bytes_accessed=moved, transcendentals=0),
            **kwargs,
        )

    def array(*shape):
        return jax.ShapeDtypeStruct(shape, jnp.float32)

    member_bytes = 4 * fields * coef * points
    packed = []
    for first, count in plan:
        packed.append(
            call(
                functools.partial(pack_kernel, first),
                6,
                10**6,
                2 * count * member_bytes,
                in_specs=[VMEM],
                out_specs=[VMEM] * 2,
                out_shape=[array(count, 2, coef, LANES)] * 2,
            )(state)
        )
    squares = call(
        squares_kernel,
        6,
        10**9,
        10**7,
        in_specs=[VMEM],
        out_specs=VMEM,
        out_shape=array(2 * members, LANES),
    )(state)
    halos = []
    near_pairs, far_pairs = halo_pairs(lax.axis_size("gx"))
    for near, far in packed:
        near = lax.ppermute(near, "gx", near_pairs)
        far = lax.ppermute(far, "gx", far_pairs)
        halos.append((near, far))
    sums = full_sum(squares)

    per_step = 4
    steps = mine // per_step // 2
    split_shape = (per_step, coef_count, coef_count)
    high, low = [], []
    for h in range(2):
        out = call(
            split_kernel,
            8,
            10**7,
            4 * mine * coef_count**2,
            grid=(steps,),
            in_specs=[pl.BlockSpec(split_shape, lambda i, h=h: (h * steps + i, 0, 0))],
            out_specs=[pl.BlockSpec(split_shape, lambda i: (i, 0, 0))] * 2,
            out_shape=[jax.ShapeDtypeStruct((mine // 2,) + split_shape[1:], jnp.bfloat16)] * 2,
        )(inverse)
        high.append(out[0])
        low.append(out[1])

    outputs = []
    for g, (first, count) in enumerate(plan):
        rows = count * fields // 2
        own = call(
            functools.partial(own_kernel, first, parts),
            8,
            3 * 2 * 2 * (2 * MODES) * (2 * LANES) * count * coef,
            2 * count * member_bytes,
            in_specs=[VMEM] * 3,
            out_specs=VMEM,
            out_shape=array(2, 2 * MODES, count * coef),
        )(state, step_high, step_low)
        sent = call(
            project_kernel,
            8,
            3 * 2 * 2 * (2 * MODES) * (4 * LANES) * count * coef,
            3 * count * member_bytes,
            in_specs=[VMEM] * 5,
            out_specs=[VMEM] * parts,
            out_shape=[array(mine * rows, LANES)] * parts,
        )(own, *halos[g], step_high, step_low)
        got = exchanged(sent, "gy")
        flops = 3 * mine * coef_count**2 * 256
        begun = call(
            functools.partial(begin_kernel, rows),
            6,
            flops,
            2 * mine * coef_count**2,
            in_specs=[VMEM] * 6,
            out_specs=VMEM,
            out_shape=array(mine * 2 * rows, coef_count),
        )(*got[:2], *high, *low)
        solved = call(
            functools.partial(solve_kernel, parts, rows),
            6,
            flops,
            2 * mine * coef_count**2,
            in_specs=[VMEM] * 8,
            out_specs=[VMEM] * parts,
            out_shape=[array((mine + 1) * rows + -(mine + 1) * rows % TILE, LANES)] * parts,
        )(*got[2:], *high, *low, begun, wall)
        returned = exchanged(solved, "gy")

        outputs = call(
            functools.partial(
                back_kernel, float(fields * coef_count * grid_x), first, mine, parts
            ),
            8,
            3 * 2 * MODES * points * count * fields * coef,
            2 * count * member_bytes,
            in_specs=[VMEM] * (parts + 3) + [ANY] * len(outputs),
            out_specs=[ANY] * 2,
            out_shape=[array(*state.shape), array(members, 2, 2, points)],
            scratch_shapes=[
                pltpu.VMEM((count, fields, coef, points), jnp.float32),
                pltpu.VMEM((count, 2, 2, points), jnp.float32),
                pltpu.SemaphoreType.DMA((count // 2 + 1,)),
            ],
            input_output_aliases={parts + 3 + i: i for i in range(len(outputs))},
        )(*returned, back_high, back_low, sums, *outputs)
    return tuple(outputs)


def solution(mesh):
    placed = (P(None, None, "gy", "gx"), P("gy", None, None))

    return jax.shard_map(
        per_device,
        mesh=mesh,
        in_specs=placed,
        out_specs=(P(None, None, "gy", "gx"), P(None, None, None, "gx")),
        check_vma=False,
    )
```
